256 devices in a mesh: phase: 8 (over y, core), row: 32 (over z, x).
Axes of the slice: x: 4, y: 4, z: 8, core: 2. Of those that a mesh axis runs over, the one named last changes fastest.
Arguments:
- linkage: float32 [2, 8, 1024, 1024], P(None, 'phase', 'row'), as said below
- pulse: float32 [32, 5, 3], replicated, may hold values from -1.2 to 1.2
- segments: int32 [8, 2], P('phase'), may hold values from 0 to 31
- ticks: int32 [8, 2], P('phase'), may hold values from 1 to 4
- detuning: float32 [5], replicated, may hold values from -0.4 to 0.4
- level_shift: float32 [5], replicated, may hold values from -1 to 1
- coupling: float32 [4], replicated, may hold values from -0.5 to 0.5
- dephase: float32 [5], replicated, may hold values from 0.01 to 0.1
Outputs:
- link_gradient: float32 [2, 8, 1024, 1024], P(None, 'phase', 'row')
The draws below stay inside these ranges and needn't reach their ends.
Inputs may be any that keep to these rules, and one draw needn't show every extreme that they name: Every linkage state is Hermitian: for each phase, the real part is a symmetric matrix and the imaginary part an antisymmetric one.
All inputs are finite; a program needn't handle non-finite values.
Results may differ from the reference program's by a relative error of at most 0.0003.
Values sent between devices are 32-bit elements; how exact they have to be, the bound alone decides.
No kernel may reach another device: no remote copies, remote signals or barrier semaphores. Data moves between devices by JAX's collectives and lax.ppermute only.
A program may use at most 64 MiB of HBM per device.

```python
import math
import jax
import jax.numpy as jnp
from jax import lax

TRANSMONS = 5
LEVELS = 4
STEPS = 2
SEGMENTS = 32
ORDER = 1024
HALF = 2
PHASES = 8


def draw_linkage(key, part):
    first_key = jax.random.fold_in(key, 11)
    second_key = jax.random.fold_in(key, 23)
    real_draw = jax.random.normal(first_key, (PHASES, ORDER, ORDER), jnp.float32)
    imag_draw = jax.random.normal(second_key, (PHASES, ORDER, ORDER), jnp.float32)
    real_component = (real_draw + jnp.swapaxes(real_draw, 1, 2)) * 0.7071067811865476
    imaginary_component = (imag_draw - jnp.swapaxes(imag_draw, 1, 2)) * 0.7071067811865476
    return jnp.stack([real_component, imaginary_component]).astype(jnp.float32)


def plant(array, rng, least, largest):
    spot = [jax.random.randint(jax.random.fold_in(rng, axis), (), 0, length) for axis, length in enumerate(array.shape)]
    main_axis = array.shape.index(max(array.shape))
    beside = spot[:main_axis] + [(spot[main_axis] + 1) % array.shape[main_axis]] + spot[main_axis + 1:]
    return array.at[tuple(spot)].set(least).at[tuple(beside)].set(largest)


def setup_inputs(seed: int = 0) -> dict:
    splits = jax.random.split(jax.random.key(seed), 9)
    linkage = draw_linkage(jax.random.fold_in(splits[8], 71), 0)
    pulse = jnp.clip(jax.random.uniform(splits[1], (SEGMENTS, TRANSMONS, LEVELS - 1), jnp.float32, -1.2, 1.2), -1.2, 1.2)
    segments = plant(jax.random.randint(splits[2], (PHASES, STEPS), 0, SEGMENTS), jax.random.fold_in(splits[2], 1), 0, SEGMENTS - 1).astype(jnp.int32)
    ticks = plant(jax.random.randint(splits[3], (PHASES, STEPS), 1, 5), jax.random.fold_in(splits[3], 1), 1, 4).astype(jnp.int32)
    detuning = jnp.clip(jax.random.uniform(splits[4], (TRANSMONS,), jnp.float32, -0.4, 0.4), -0.4, 0.4)
    level_shift = jnp.clip(jax.random.uniform(splits[5], (TRANSMONS,), jnp.float32, -1.0, 1.0), -1.0, 1.0)
    coupling = jnp.clip(jax.random.uniform(splits[6], (TRANSMONS - 1,), jnp.float32, -0.5, 0.5), -0.5, 0.5)
    dephase = jnp.clip(jnp.exp(jax.random.uniform(splits[7], (TRANSMONS,), jnp.float32, math.log(0.01), math.log(0.1))), 0.01, 0.1)
    return {"linkage": linkage, "pulse": pulse, "segments": segments, "ticks": ticks, "detuning": detuning, "level_shift": level_shift, "coupling": coupling, "dephase": dephase}


TOP_ACCURACY = lax.Precision.HIGHEST


def digits(indices):
    powers = LEVELS ** (TRANSMONS - 1 - jnp.arange(TRANSMONS, dtype=jnp.int32))
    return ((indices[None, :] // powers[:, None]) % LEVELS).astype(jnp.float32)


def energies(levels, level_shift, coupling):
    own_part = jnp.sum(level_shift[:, None] * levels * (levels - 1.0) * 0.5, axis=0)
    return own_part + jnp.sum(coupling[:, None] * levels[:-1] * levels[1:], axis=0)


def drift_tables(row_levels, col_levels, level_shift, coupling, dephase):
    detune_grid = energies(row_levels, level_shift, coupling)[:, None] - energies(col_levels, level_shift, coupling)[None, :]
    weighted = dephase[:, None] * row_levels
    cross = jnp.dot(weighted.T, col_levels, preferred_element_type=jnp.float32, precision=TOP_ACCURACY)
    row_part = jnp.sum(weighted * row_levels, axis=0)
    col_part = jnp.sum(dephase[:, None] * col_levels * col_levels, axis=0)
    decay = row_part[:, None] + col_part[None, :] - 2.0 * cross
    return decay, detune_grid


def half_factor(decay, detune_grid, span):
    magnitude = jnp.exp(-0.5 * span * decay)
    return magnitude * jnp.cos(0.5 * span * detune_grid), -magnitude * jnp.sin(0.5 * span * detune_grid)


def weigh(field, factor_real, factor_imag):
    return jnp.stack([field[0] * factor_real - field[1] * factor_imag, field[0] * factor_imag + field[1] * factor_real])


def complex_product(left_real_component, left_imaginary, right_real_component, right_imaginary):
    real_component = jnp.einsum('nmx,nxw->nmw', left_real_component, right_real_component, precision=TOP_ACCURACY) - jnp.einsum('nmx,nxw->nmw', left_imaginary, right_imaginary, precision=TOP_ACCURACY)
    imaginary_component = jnp.einsum('nmx,nxw->nmw', left_real_component, right_imaginary, precision=TOP_ACCURACY) + jnp.einsum('nmx,nxw->nmw', left_imaginary, right_real_component, precision=TOP_ACCURACY)
    return real_component, imaginary_component


def rotations(theta, phi):
    identity = jnp.eye(LEVELS, dtype=jnp.float32)
    total_real = jnp.broadcast_to(identity, (theta.shape[0], LEVELS, LEVELS))
    total_imag = jnp.zeros((theta.shape[0], LEVELS, LEVELS), jnp.float32)
    for level in range(LEVELS - 1):
        upper = jnp.outer(identity[level], identity[level + 1])
        lower = upper.T
        block = jnp.outer(identity[level], identity[level]) + jnp.outer(identity[level + 1], identity[level + 1])
        cosine = jnp.cos(theta[:, level])[:, None, None]
        sine = jnp.sin(theta[:, level])[:, None, None]
        phase_cos = jnp.cos(phi[:, level])[:, None, None]
        phase_sin = jnp.sin(phi[:, level])[:, None, None]
        rot_real = identity + (cosine - 1.0) * block + sine * phase_cos * (lower - upper)
        rot_imag = sine * phase_sin * (upper + lower)
        total_real, total_imag = complex_product(total_real, total_imag, rot_real, rot_imag)
    return total_real, total_imag


def kron_range(unit_real, unit_imag, first, last):
    acc_real, acc_imag = unit_real[first], unit_imag[first]
    for transmon in range(first + 1, last):
        next_real, next_imag = unit_real[transmon], unit_imag[transmon]
        acc_real, acc_imag = (jnp.kron(acc_real, next_real) - jnp.kron(acc_imag, next_imag),
                              jnp.kron(acc_real, next_imag) + jnp.kron(acc_imag, next_real))
    return acc_real, acc_imag


def real_form(matrix_real, matrix_imag):
    return jnp.stack([jnp.stack([matrix_real, -matrix_imag], axis=1), jnp.stack([matrix_imag, matrix_real], axis=1)], axis=0)


def factor_forms(unit_real, unit_imag, grouped):
    if grouped:
        pairs = [kron_range(unit_real, unit_imag, 0, HALF), kron_range(unit_real, unit_imag, HALF, TRANSMONS)]
    else:
        pairs = [(unit_real[transmon], unit_imag[transmon]) for transmon in range(TRANSMONS)]
    forward_left = [real_form(matrix_real, matrix_imag) for matrix_real, matrix_imag in pairs]
    forward_right = [real_form(matrix_real, -matrix_imag) for matrix_real, matrix_imag in pairs]
    adjoint_left = [real_form(matrix_real.T, -matrix_imag.T) for matrix_real, matrix_imag in pairs]
    adjoint_right = [real_form(matrix_real.T, matrix_imag.T) for matrix_real, matrix_imag in pairs]
    return forward_left, forward_right, adjoint_left, adjoint_right


def apply_factor(field, form, leading, trailing):
    width = form.shape[3]
    shaped = field.reshape(2, leading, width, trailing)
    result = jnp.einsum('cgdf,dpfq->cpgq', form, shaped, precision=TOP_ACCURACY)
    return result.reshape(field.shape)


def apply_factors(field, forms, leading, trailing):
    widths = [form.shape[3] for form in forms]
    for position, form in enumerate(forms):
        before = math.prod(widths[:position])
        after = math.prod(widths[position + 1:])
        field = apply_factor(field, form, leading * before, after * trailing)
    return field


def step_unitaries(pulse, segment, clock, span, detuning):
    onehot = (jnp.arange(SEGMENTS, dtype=jnp.int32) == segment).astype(jnp.float32)
    theta = jnp.einsum('s,skm->km', onehot, pulse, precision=TOP_ACCURACY)
    multiple = jnp.arange(1, LEVELS, dtype=jnp.int32).astype(jnp.float32)
    phi = detuning[:, None] * (clock + 0.5 * span) * multiple[None, :]
    return rotations(theta, phi)


def full_sandwich(field, left_forms, right_forms):
    field = apply_factors(field, left_forms, 1, ORDER)
    return apply_factors(field, right_forms, ORDER, 1)


def reference(linkage, pulse, segments, ticks, detuning, level_shift, coupling, dephase):
    levels = digits(jnp.arange(ORDER, dtype=jnp.int32))
    decay, detune_grid = drift_tables(levels, levels, level_shift, coupling, dephase)
    totals = jnp.sum(ticks, axis=1, dtype=jnp.int32)
    starts = (jnp.cumsum(totals, dtype=jnp.int32) - totals).astype(jnp.int32)

    def prepared(phase_index, step_index):
        span = ticks[phase_index, step_index].astype(jnp.float32)
        earlier = jnp.sum(ticks[phase_index, :step_index], dtype=jnp.int32)
        clock = (starts[phase_index] + earlier).astype(jnp.float32)
        unit_real, unit_imag = step_unitaries(pulse, segments[phase_index, step_index], clock, span, detuning)
        return span, factor_forms(unit_real, unit_imag, True)

    def forward(phase_index):
        field = linkage[:, phase_index]
        for step_index in range(STEPS):
            span, forms = prepared(phase_index, step_index)
            factor_real, factor_imag = half_factor(decay, detune_grid, span)
            field = weigh(field, factor_real, factor_imag)
            field = full_sandwich(field, forms[0], forms[1])
            field = weigh(field, factor_real, factor_imag)
        return field

    phase_ids = jnp.arange(PHASES, dtype=jnp.int32)
    ends = jnp.moveaxis(lax.map(forward, phase_ids), 0, 1)
    mismatch = ends - jnp.roll(linkage, -1, axis=1)

    def backward(phase_index):
        field = mismatch[:, phase_index]
        for step_index in reversed(range(STEPS)):
            span, forms = prepared(phase_index, step_index)
            factor_real, factor_imag = half_factor(decay, detune_grid, span)
            field = weigh(field, factor_real, -factor_imag)
            field = full_sandwich(field, forms[2], forms[3])
            field = weigh(field, factor_real, -factor_imag)
        return field

    adjoints = jnp.moveaxis(lax.map(backward, phase_ids), 0, 1)
    return adjoints - jnp.roll(mismatch, 1, axis=1)
```

```python
import math

import jax
import jax.numpy as jnp
from jax import lax
from jax.experimental import pallas as pl
from jax.experimental.pallas import tpu as pltpu
from jax.sharding import PartitionSpec as P

TRANSMONS = 5
LEVELS = 4
STEPS = 2


F32 = jnp.float32
BF16 = jnp.bfloat16


def iota(shape, dim):
    return lax.broadcasted_iota(jnp.int32, shape, dim)


def sincos(x):
    q = jnp.floor(x * F32(2.0 / math.pi) + F32(0.5))
    r = x - q * F32(1.5703125)
    r = r - q * F32(4.837512969970703125e-4)
    r = r - q * F32(7.549789948768648e-8)
    z = r * r
    s = r + r * z * (F32(-1 / 6) + z * (F32(1 / 120) + z * (F32(-1 / 5040) + z * F32(1 / 362880))))
    c = F32(1.0) + z * (
        F32(-0.5) + z * (F32(1 / 24) + z * (F32(-1 / 720) + z * F32(1 / 40320)))
    )
    k = q.astype(jnp.int32)
    odd = (k & 1) == 1
    sin = jnp.where(odd, c, s)
    cos = jnp.where(odd, s, c)
    sin = jnp.where((k & 2) == 2, -sin, sin)
    cos = jnp.where(((k + 1) & 2) == 2, -cos, cos)
    return sin, cos


def split(x):
    hi = x.astype(BF16)
    return hi, (x - hi.astype(F32)).astype(BF16)


def dot(a, b, transposed=False):
    dims = (((1,), (1 if transposed else 0,)), ((), ()))
    return lax.dot_general(a, b, dims, preferred_element_type=F32)


def mm(x, hi, lo, transposed=False):
    a, b = split(x)
    return dot(a, hi, transposed) + dot(a, lo, transposed) + dot(b, hi, transposed)


def left(hi, lo, x):
    a, b = split(x)
    return dot(hi, a) + dot(hi, b) + dot(lo, a)


def pmm(x, w, transposed=False):
    a, b = split(x)
    return dot(a, w, transposed) + dot(b, w, transposed)


def pleft(w, x):
    a, b = split(x)
    return dot(w, a) + dot(w, b)


def rotation(ints, pulse, step, k, width):
    base = ints[step] * 15 + 3 * k
    sc = [sincos(jnp.full((1, width), pulse[base + m], F32)) for m in range(3)]
    (s0, c0), (s1, c1), (s2, c2) = sc
    zero = jnp.zeros((1, width), F32)
    return [
        [c0, -s0 * c1, s0 * s1 * c2, -s0 * s1 * s2],
        [s0, c0 * c1, -c0 * s1 * c2, c0 * s1 * s2],
        [zero, s1, c1 * c2, -c1 * s2],
        [zero, zero, s2, c2],
    ]


def identity(width):
    one, zero = jnp.ones((1, width), F32), jnp.zeros((1, width), F32)
    return [[one if a == b else zero for b in range(4)] for a in range(4)]


def flip(o):
    return [[o[b][a] for b in range(4)] for a in range(4)]


def pick(digit, choices):
    out = choices[3]
    for v in (2, 1, 0):
        out = jnp.where(digit == v, choices[v], out)
    return out


def lane_rows(o, lane_digit):
    return [pick(lane_digit, o[x]) for x in range(4)]


def kron_blocks(mats, lane_digits):
    width = lane_digits[0].shape[1]
    t = [lane_rows(o, d) for o, d in zip(mats, lane_digits)]
    row = iota((16, width), 0)
    low = pick(row >> 2, t[2]) * pick(row & 3, t[3])
    return [low * (t[0][a] * t[1][b]) for a in range(4) for b in range(4)]


def store_kron(hi_ref, lo_ref, mats, lane_digits):
    for n, block in enumerate(kron_blocks(mats, lane_digits)):
        hi, lo = split(block)
        hi_ref[16 * n : 16 * n + 16, :] = hi
        if lo_ref is not None:
            lo_ref[16 * n : 16 * n + 16, :] = lo


def small_table(row_digits, lane_digits, mats):
    out = None
    for o, rd, ld in zip(mats, row_digits, lane_digits):
        part = pick(rd, lane_rows(o, ld))
        out = part if out is None else out * part
    return out


def fnum(x):
    return x.astype(F32)


def node_energy(fl, k, n):
    return fl[k] * (n * (n - F32(1.0)) * F32(0.5))


def drive_weight(n):
    return n * (n + F32(1.0)) * F32(0.5)


def table_a_kernel(ints, fl, pulse, w1h, w1l, w2h, w2l, wp, r1, r2, far, fai, o0):
    w = 256
    lane = iota((1, w), 1)
    natural = [(lane >> 6) & 3, (lane >> 4) & 3, (lane >> 2) & 3, lane & 3]
    moved = [
        (lane >> 3) & 3,
        (lane >> 1) & 3,
        (lane >> 6) & 3,
        ((lane >> 5) & 1) * 2 + (lane & 1),
    ]
    eye = identity(w)
    first = [rotation(ints, pulse, 0, k, w) for k in range(TRANSMONS)]
    second = {k: rotation(ints, pulse, 1, k, w) for k in (3, 4)}
    store_kron(w1h, w1l, [flip(first[k]) for k in (1, 2, 3, 4)], natural)
    store_kron(w2h, w2l, [eye, eye, flip(second[3]), flip(second[4])], moved)
    store_kron(wp, None, [eye] * 4, moved)
    for a in range(4):
        for b in range(4):
            o0[4 * a + b : 4 * a + b + 1, :] = first[0][a][b]
    rl = iota((1, 32), 1)
    rr = iota((32, 32), 0)
    one = [[e[:, :32] for e in row] for row in eye]
    f3 = [[e[:, :32] for e in row] for row in first[3]]
    f4 = [[e[:, :32] for e in row] for row in first[4]]
    g4 = [[e[:, :32] for e in row] for row in second[4]]
    nat_r = [rr >> 4, (rr >> 2) & 3, rr & 3]
    nat_l = [rl >> 4, (rl >> 2) & 3, rl & 3]
    mov_r = [(rr >> 2) & 1, rr & 3, rr >> 3]
    mov_l = [(rl >> 2) & 1, rl & 3, rl >> 3]
    tables = [
        small_table(nat_r, nat_l, [one, f3, f4]),
        small_table(nat_r, nat_l, [one, flip(f3), flip(f4)]),
    ]
    for n, t in enumerate(tables):
        hi, lo = split(t)
        r1[2 * n], r1[2 * n + 1] = hi, lo
    tables = [
        small_table(mov_r, nat_l, [one, one, g4]),
        small_table(nat_r, mov_l, [one, one, flip(g4)]),
        small_table(mov_r, nat_l, [one, one, one]),
        small_table(nat_r, mov_l, [one, one, one]),
    ]
    for n, t in enumerate(tables):
        hi, lo = split(t)
        r2[2 * n], r2[2 * n + 1] = hi, lo
    t12 = F32(0.5) * (fnum(ints[2]) + fnum(ints[3]))
    row = iota((32, 128), 0)
    col = iota((1, 128), 1)
    i3, i4 = fnum((row >> 2) & 3), fnum(row & 3)
    j2, j3, j4 = fnum((col >> 4) & 3), fnum((col >> 2) & 3), fnum(col & 3)

    def node(k, n):
        return node_energy(fl, k, n) + fl[14 + k] * drive_weight(n)

    ai = t12 * (fl[8] * (i3 * i4) + node(4, i4))
    aj = t12 * (fl[7] * (j2 * j3) + fl[8] * (j3 * j4) + node(3, j3) + node(4, j4))
    mag = jnp.exp(
        -t12 * (fl[12] * ((i3 - j3) * (i3 - j3)) + fl[13] * ((i4 - j4) * (i4 - j4)))
    )
    si, ci = sincos(ai)
    sj, cj = sincos(aj)
    far[...] = mag * (ci * cj + si * sj)
    fai[...] = mag * (ci * sj - si * cj)


def start_of(ints, gathered):
    rows = iota((8, 2), 0)
    kept = jnp.where(rows < ints[5], gathered[...], 0).astype(F32)
    return jnp.sum(jnp.sum(kept, axis=1, keepdims=True), axis=0, keepdims=True)


def drive_phase(fl, k, time):
    phi = time * fl[14 + k]
    turns = jnp.floor(phi * F32(0.5 / math.pi) + F32(0.5))
    return phi - turns * F32(6.28125) - turns * F32(2 * math.pi - 6.28125)


def energy_of(fl, digits):
    total = node_energy(fl, 0, digits[0])
    for k in range(1, TRANSMONS):
        total = total + node_energy(fl, k, digits[k])
    for k in range(TRANSMONS - 1):
        total = total + fl[5 + k] * (digits[k] * digits[k + 1])
    return total


def factor_parts(fl, span, sign, time, row_digits, col_digits):
    phis = [drive_phase(fl, k, time) for k in range(TRANSMONS)]

    def angle(digits):
        total = (F32(0.5) * span) * energy_of(fl, digits)
        drive = phis[0] * drive_weight(digits[0])
        for k in range(1, TRANSMONS):
            drive = drive + phis[k] * drive_weight(digits[k])
        return total + drive if sign > 0 else total - drive

    return sincos(angle(row_digits)), sincos(angle(col_digits))


def decay_of(fl, row_digits, col_digits):
    total = None
    for k in range(TRANSMONS):
        gap = row_digits[k] - col_digits[k]
        part = fl[9 + k] * (gap * gap)
        total = part if total is None else total + part
    return total


def first_factor(ints, fl, gathered):
    span = fnum(ints[2])
    time = start_of(ints, gathered) + F32(0.5) * span
    row = ints[4] * 32 + iota((32, 128), 0)
    col = iota((1, 1024), 1)
    rd = [fnum((row >> (8 - 2 * k)) & 3) for k in range(TRANSMONS)]
    cd = [fnum((col >> (8 - 2 * k)) & 3) for k in range(TRANSMONS)]
    (si, ci), (sj, cj) = factor_parts(fl, span, 1, time, rd, cd)
    wide = [jnp.concatenate([d] * 8, axis=1) for d in rd]
    mag = jnp.exp(F32(-0.5) * span * decay_of(fl, wide, cd))
    si, ci = jnp.concatenate([si] * 8, axis=1), jnp.concatenate([ci] * 8, axis=1)
    return mag * (ci * cj + si * sj), mag * (ci * sj - si * cj)


def to_rows(blocks):
    return jnp.concatenate(
        [
            blocks[:, c * 1024 + a * 256 : c * 1024 + a * 256 + 256]
            for a in range(4)
            for c in range(2)
        ],
        axis=0,
    )


def to_lanes(rows):
    return jnp.concatenate(
        [rows[(2 * a + c) * 32 : (2 * a + c) * 32 + 32, :] for c in range(2) for a in range(4)],
        axis=1,
    )


def mix_top(o0, rows, transposed):
    out = []
    for a in range(4):
        total = None
        for b in range(4):
            n = 4 * b + a if transposed else 4 * a + b
            part = rows[64 * b : 64 * b + 64, :] * o0[n : n + 1, :]
            total = part if total is None else total + part
        out.append(total)
    return jnp.concatenate(out, axis=0)


def chunk_of_lane(shape):
    return (iota(shape, 1) >> 5) & 3


def send(out, offset, x):
    for c in range(2):
        for half in range(2):
            tiles = [
                x[:, c * 1024 + a * 256 + half * 128 : c * 1024 + a * 256 + half * 128 + 128]
                for a in range(4)
            ]
            chunk = chunk_of_lane((32, 128))
            for q in range(4):
                moved = [
                    tiles[a] if a == q else pltpu.roll(tiles[a], ((a - q) * 32) % 128, 1)
                    for a in range(4)
                ]
                merged = pick(chunk, moved)
                for i4 in range(4):
                    out[i4 * 8 + half * 4 + q, :, offset + c * 128 : offset + c * 128 + 128] = (
                        merged[i4 * 8 : i4 * 8 + 8, :]
                    )


def receive(ref, offset):
    chunk = chunk_of_lane((32, 128))
    pieces = {}
    for c in range(2):
        for half in range(2):
            merged = [
                jnp.concatenate(
                    [
                        ref[i4 * 8 + half * 4 + q, :, offset + c * 128 : offset + c * 128 + 128]
                        for i4 in range(4)
                    ],
                    axis=0,
                )
                for q in range(4)
            ]
            for a in range(4):
                moved = [
                    merged[q] if a == q else pltpu.roll(merged[q], ((q - a) * 32) % 128, 1)
                    for q in range(4)
                ]
                pieces[c, a, half] = pick(chunk, moved)
    return jnp.concatenate(
        [pieces[c, a, half] for c in range(2) for a in range(4) for half in range(2)], axis=1
    )


def apply_pointwise_a(rows, far, fai, conj):
    fr = jnp.concatenate([far, far], axis=1)
    fi = jnp.concatenate([fai, fai], axis=1)
    if conj:
        fi = -fi
    out = []
    for a in range(4):
        re, im = rows[64 * a : 64 * a + 32, :], rows[64 * a + 32 : 64 * a + 64, :]
        out += [re * fr - im * fi, re * fi + im * fr]
    return jnp.concatenate(out, axis=0)


def forward_a_kernel(
    ints, fl, gathered, x, f, w1h, w1l, w2h, w2l, wp, r1, r2, far, fai, o0, out
):
    fr, fi = first_factor(ints, fl, gathered)
    re, im = x[0], x[1]
    both = jnp.concatenate([re * fr - im * fi, re * fi + im * fr], axis=1)
    both = left(r1[0], r1[1], both)
    rows = mix_top(o0, to_rows(both), False)
    rows = mm(rows, w1h[...], w1l[...])
    rows = apply_pointwise_a(rows, far[...], fai[...], False)
    rows = mm(rows, w2h[...], w2l[...])
    send(out, 0, left(r2[0], r2[1], to_lanes(rows)))
    rows = to_rows(jnp.concatenate([f[0], f[1]], axis=1))
    send(out, 256, pleft(r2[4], to_lanes(pmm(rows, wp[...]))))


def adjoint_a_kernel(
    ints, fl, gathered, y, m, w1h, w1l, w2h, w2l, wp, r1, r2, far, fai, o0, out
):
    rows = to_rows(left(r2[2], r2[3], receive(y, 0)))
    rows = mm(rows, w2h[...], w2l[...], True)
    rows = apply_pointwise_a(rows, far[...], fai[...], True)
    rows = mm(rows, w1h[...], w1l[...], True)
    rows = mix_top(o0, rows, True)
    both = left(r1[2], r1[3], to_lanes(rows))
    fr, fi = first_factor(ints, fl, gathered)
    re, im = both[:, :1024], both[:, 1024:]
    other = to_lanes(pmm(to_rows(pleft(r2[6], receive(m, 0))), wp[...], True))
    out[0] = re * fr + im * fi - other[:, :1024]
    out[1] = im * fr - re * fi - other[:, 1024:]


def table_b_kernel(
    ints, fl, gathered, pulse, a1h, a1l, b1h, b1l, a2h, a2l, b2h, b2l, vh, vl, fmr, fmi, ffr, ffi
):
    w = 256
    lane = iota((1, w), 1)
    natural = [(lane >> 6) & 3, (lane >> 4) & 3, (lane >> 2) & 3, lane & 3]
    eye = identity(w)
    first = [rotation(ints, pulse, 0, k, w) for k in range(3)]
    second = [rotation(ints, pulse, 1, k, w) for k in range(4)]
    store_kron(a1h, a1l, [*first, eye], natural)
    store_kron(b1h, b1l, [*(flip(o) for o in first), eye], natural)
    store_kron(a2h, a2l, second, natural)
    store_kron(b2h, b2l, [flip(o) for o in second], natural)
    row = iota((16, w), 0)
    cl, l0, l1, l2, ll = (lane >> 7), (lane >> 5) & 3, (lane >> 3) & 3, (lane >> 1) & 3, lane & 1
    t0 = lane_rows(flip(second[0]), l0)
    t1 = lane_rows(flip(second[1]), l1)
    t2 = lane_rows(flip(second[2]), l2)
    low = pick((row >> 1) & 3, t2) * jnp.where((row & 1) == ll, F32(1.0), F32(0.0))
    high_bit = row >> 3
    for n in range(16):
        c, d0, top = n >> 3, (n >> 1) & 3, n & 1
        mid = jnp.where(high_bit == 0, t1[2 * top], t1[2 * top + 1])
        block = low * mid * (t0[d0] * jnp.where(cl == c, F32(1.0), F32(0.0)))
        hi, lo = split(block)
        vh[16 * n : 16 * n + 16, :] = hi
        vl[16 * n : 16 * n + 16, :] = lo
    row = iota((256, 128), 0)
    col = iota((1, 128), 1)
    rd = [fnum((row >> (6 - 2 * k)) & 3) for k in range(4)]
    cd = [fnum((col >> 5) & 3), fnum((col >> 3) & 3), fnum((col >> 1) & 3)]
    t12 = F32(0.5) * (fnum(ints[2]) + fnum(ints[3]))

    def node(k, n):
        return node_energy(fl, k, n) + fl[14 + k] * drive_weight(n)

    ai = fl[5] * (rd[0] * rd[1]) + fl[6] * (rd[1] * rd[2]) + fl[7] * (rd[2] * rd[3])
    for k in range(4):
        ai = ai + node(k, rd[k])
    aj = fl[5] * (cd[0] * cd[1]) + fl[6] * (cd[1] * cd[2])
    for k in range(3):
        aj = aj + node(k, cd[k])
    gap = None
    for k in range(3):
        part = fl[9 + k] * ((rd[k] - cd[k]) * (rd[k] - cd[k]))
        gap = part if gap is None else gap + part
    mag = jnp.exp(-t12 * gap)
    si, ci = sincos(t12 * ai)
    sj, cj = sincos(t12 * aj)
    fmr[...] = mag * (ci * cj + si * sj)
    fmi[...] = mag * (ci * sj - si * cj)
    rank = ints[4]
    i4 = fnum(jnp.full((256, 128), rank >> 3, jnp.int32))
    j3 = fnum(jnp.full((1, 128), (rank >> 1) & 3, jnp.int32))
    j4 = fnum((rank & 1) * 2 + (col & 1))
    rows = [*rd, i4]
    cols = [*cd, j3, j4]
    span = fnum(ints[3])
    time = start_of(ints, gathered) + (fnum(ints[2]) + F32(0.5) * span)
    (si, ci), (sj, cj) = factor_parts(fl, span, -1, time, rows, cols)
    mag = jnp.exp(F32(-0.5) * span * decay_of(fl, rows, cols))
    ffr[...] = mag * (ci * cj + si * sj)
    ffi[...] = mag * (ci * sj - si * cj)


def cmul(x, fr, fi, conj=False):
    re, im = x[:, :128], x[:, 128:]
    if conj:
        return jnp.concatenate([re * fr + im * fi, im * fr - re * fi], axis=1)
    return jnp.concatenate([re * fr - im * fi, re * fi + im * fr], axis=1)


def both_b_kernel(x, a1h, a1l, b1h, b1l, a2h, a2l, b2h, b2l, vh, vl, fmr, fmi, ffr, ffi, out):
    z = left(a1h[...], a1l[...], x[:, :256])
    z = cmul(z, fmr[...], fmi[...])
    z = left(a2h[...], a2l[...], z)
    z = mm(z, vh[...], vl[...])
    z = cmul(z, ffr[...], ffi[...]) - x[:, 256:]
    out[:, 256:] = z
    z = cmul(z, ffr[...], ffi[...], True)
    z = left(b2h[...], b2l[...], z)
    z = mm(z, vh[...], vl[...], True)
    z = cmul(z, fmr[...], fmi[...], True)
    out[:, :256] = left(b1h[...], b1l[...], z)


SMEM = pl.BlockSpec(memory_space=pltpu.SMEM)
VMEM = pl.BlockSpec(memory_space=pltpu.VMEM)


def call(kernel, args, scalars, outs, flops, name):
    specs = [SMEM if n in scalars else VMEM for n in range(len(args))]
    return pl.pallas_call(
        kernel,
        in_specs=specs,
        out_specs=jax.tree.map(lambda _: VMEM, outs),
        out_shape=outs,
        name=name,
        cost_estimate=pl.CostEstimate(flops=flops, transcendentals=0, bytes_accessed=1 << 20),
    )(*args)


def sds(*shape, dtype=F32):
    return jax.ShapeDtypeStruct(shape, dtype)


def local(linkage, pulse, segments, ticks, detuning, level_shift, coupling, dephase):
    current = linkage[:, 0]
    phases = lax.axis_size("phase")
    ints = jnp.concatenate(
        [
            segments[0],
            ticks[0],
            jnp.stack([lax.axis_index("row"), lax.axis_index("phase")]).astype(jnp.int32),
        ]
    )
    floats = jnp.concatenate([level_shift, coupling, dephase, detuning])
    flat_pulse = pulse.reshape(-1)
    gathered = lax.all_to_all(
        jnp.broadcast_to(ticks, (phases, STEPS)), "phase", split_axis=0, concat_axis=0, tiled=True
    )
    following = lax.ppermute(
        current, "phase", [((i + 1) % phases, i) for i in range(phases)]
    )
    square = sds(256, 256, dtype=BF16)
    tables_a = call(
        table_a_kernel,
        (ints, floats, flat_pulse),
        (0, 1, 2),
        (
            *([square] * 5),
            sds(4, 32, 32, dtype=BF16),
            sds(8, 32, 32, dtype=BF16),
            sds(32, 128),
            sds(32, 128),
            sds(16, 256),
        ),
        1 << 28,
        "table_a",
    )
    sent = call(
        forward_a_kernel,
        (ints, floats, gathered, current, following, *tables_a),
        (0, 1),
        sds(32, 8, 512),
        1 << 28,
        "forward_a",
    )
    turned = lax.all_to_all(sent, "row", split_axis=0, concat_axis=0, tiled=True)
    tables_b = call(
        table_b_kernel,
        (ints, floats, gathered, flat_pulse),
        (0, 1, 3),
        (*([square] * 10), *([sds(256, 128)] * 4)),
        1 << 30,
        "table_b",
    )
    back = call(
        both_b_kernel,
        (turned.reshape(256, 512), *tables_b),
        (),
        sds(256, 512),
        1 << 28,
        "both_b",
    )
    returned = lax.all_to_all(
        back.reshape(32, 8, 512), "row", split_axis=0, concat_axis=0, tiled=True
    )
    earlier = lax.ppermute(
        returned[:, :, 256:], "phase", [(i, (i + 1) % phases) for i in range(phases)]
    )
    result = call(
        adjoint_a_kernel,
        (ints, floats, gathered, returned, earlier, *tables_a),
        (0, 1),
        sds(2, 32, 1024),
        1 << 28,
        "adjoint_a",
    )
    return result[:, None]


def solution(mesh):
    return jax.shard_map(
        local,
        mesh=mesh,
        in_specs=(
            P(None, "phase", "row", None),
            P(),
            P("phase", None),
            P("phase", None),
            P(),
            P(),
            P(),
            P(),
        ),
        out_specs=P(None, "phase", "row", None),
        check_vma=False,
    )
```

```python
import math

import jax
import jax.numpy as jnp
from jax import lax
from jax.experimental import pallas as pl
from jax.experimental.pallas import tpu as pltpu
from jax.sharding import PartitionSpec as P

TRANSMONS = 5
LEVELS = 4
STEPS = 2


F32 = jnp.float32
BF16 = jnp.bfloat16


def iota(shape, dim):
    return lax.broadcasted_iota(jnp.int32, shape, dim)


def sincos(x):
    q = jnp.floor(x * F32(2.0 / math.pi) + F32(0.5))
    r = x - q * F32(1.5703125)
    r = r - q * F32(4.837512969970703125e-4)
    r = r - q * F32(7.549789948768648e-8)
    z = r * r
    s = r + r * z * (F32(-1 / 6) + z * (F32(1 / 120) + z * (F32(-1 / 5040) + z * F32(1 / 362880))))
    c = F32(1.0) + z * (
        F32(-0.5) + z * (F32(1 / 24) + z * (F32(-1 / 720) + z * F32(1 / 40320)))
    )
    k = q.astype(jnp.int32)
    odd = (k & 1) == 1
    sin = jnp.where(odd, c, s)
    cos = jnp.where(odd, s, c)
    sin = jnp.where((k & 2) == 2, -sin, sin)
    cos = jnp.where(((k + 1) & 2) == 2, -cos, cos)
    return sin, cos


def split(x):
    hi = x.astype(BF16)
    return hi, (x - hi.astype(F32)).astype(BF16)


def dot(a, b, transposed=False):
    dims = (((1,), (1 if transposed else 0,)), ((), ()))
    return lax.dot_general(a, b, dims, preferred_element_type=F32)


def mm(x, hi, lo, transposed=False):
    a, b = split(x)
    return dot(a, hi, transposed) + dot(a, lo, transposed) + dot(b, hi, transposed)


def left(hi, lo, x):
    a, b = split(x)
    return dot(hi, a) + dot(hi, b) + dot(lo, a)


def pmm(x, w, transposed=False):
    a, b = split(x)
    return dot(a, w, transposed) + dot(b, w, transposed)


def pleft(w, x):
    a, b = split(x)
    return dot(w, a) + dot(w, b)


def rotation(ints, pulse, step, k, width):
    base = ints[step] * 15 + 3 * k
    sc = [sincos(jnp.full((1, width), pulse[base + m], F32)) for m in range(3)]
    (s0, c0), (s1, c1), (s2, c2) = sc
    zero = jnp.zeros((1, width), F32)
    return [
        [c0, -s0 * c1, s0 * s1 * c2, -s0 * s1 * s2],
        [s0, c0 * c1, -c0 * s1 * c2, c0 * s1 * s2],
        [zero, s1, c1 * c2, -c1 * s2],
        [zero, zero, s2, c2],
    ]


def identity(width):
    one, zero = jnp.ones((1, width), F32), jnp.zeros((1, width), F32)
    return [[one if a == b else zero for b in range(4)] for a in range(4)]


def flip(o):
    return [[o[b][a] for b in range(4)] for a in range(4)]


def pick(digit, choices):
    out = choices[3]
    for v in (2, 1, 0):
        out = jnp.where(digit == v, choices[v], out)
    return out


def lane_rows(o, lane_digit):
    return [pick(lane_digit, o[x]) for x in range(4)]


def kron_blocks(mats, lane_digits):
    width = lane_digits[0].shape[1]
    t = [lane_rows(o, d) for o, d in zip(mats, lane_digits)]
    row = iota((16, width), 0)
    low = pick(row >> 2, t[2]) * pick(row & 3, t[3])
    return [low * (t[0][a] * t[1][b]) for a in range(4) for b in range(4)]


def store_kron(hi_ref, lo_ref, mats, lane_digits):
    for n, block in enumerate(kron_blocks(mats, lane_digits)):
        hi, lo = split(block)
        hi_ref[16 * n : 16 * n + 16, :] = hi
        if lo_ref is not None:
            lo_ref[16 * n : 16 * n + 16, :] = lo


def small_table(row_digits, lane_digits, mats):
    out = None
    for o, rd, ld in zip(mats, row_digits, lane_digits):
        part = pick(rd, lane_rows(o, ld))
        out = part if out is None else out * part
    return out


def fnum(x):
    return x.astype(F32)


def node_energy(fl, k, n):
    return fl[k] * (n * (n - F32(1.0)) * F32(0.5))


def drive_weight(n):
    return n * (n + F32(1.0)) * F32(0.5)


def table_a_kernel(ints, fl, pulse, w1h, w1l, w2h, w2l, wp, r1, r2, far, fai, o0):
    w = 256
    lane = iota((1, w), 1)
    natural = [(lane >> 6) & 3, (lane >> 4) & 3, (lane >> 2) & 3, lane & 3]
    moved = [
        (lane >> 3) & 3,
        (lane >> 1) & 3,
        (lane >> 6) & 3,
        ((lane >> 5) & 1) * 2 + (lane & 1),
    ]
    eye = identity(w)
    first = [rotation(ints, pulse, 0, k, w) for k in range(TRANSMONS)]
    second = {k: rotation(ints, pulse, 1, k, w) for k in (3, 4)}
    store_kron(w1h, w1l, [flip(first[k]) for k in (1, 2, 3, 4)], natural)
    store_kron(w2h, w2l, [eye, eye, flip(second[3]), flip(second[4])], moved)
    store_kron(wp, None, [eye] * 4, moved)
    for a in range(4):
        for b in range(4):
            o0[4 * a + b : 4 * a + b + 1, :] = first[0][a][b]
    rl = iota((1, 32), 1)
    rr = iota((32, 32), 0)
    one = [[e[:, :32] for e in row] for row in eye]
    f3 = [[e[:, :32] for e in row] for row in first[3]]
    f4 = [[e[:, :32] for e in row] for row in first[4]]
    g4 = [[e[:, :32] for e in row] for row in second[4]]
    nat_r = [rr >> 4, (rr >> 2) & 3, rr & 3]
    nat_l = [rl >> 4, (rl >> 2) & 3, rl & 3]
    mov_r = [(rr >> 2) & 1, rr & 3, rr >> 3]
    mov_l = [(rl >> 2) & 1, rl & 3, rl >> 3]
    tables = [
        small_table(nat_r, nat_l, [one, f3, f4]),
        small_table(nat_r, nat_l, [one, flip(f3), flip(f4)]),
    ]
    for n, t in enumerate(tables):
        hi, lo = split(t)
        r1[2 * n], r1[2 * n + 1] = hi, lo
    tables = [
        small_table(mov_r, nat_l, [one, one, g4]),
        small_table(nat_r, mov_l, [one, one, flip(g4)]),
        small_table(mov_r, nat_l, [one, one, one]),
        small_table(nat_r, mov_l, [one, one, one]),
    ]
    for n, t in enumerate(tables):
        hi, lo = split(t)
        r2[2 * n], r2[2 * n + 1] = hi, lo
    t12 = F32(0.5) * (fnum(ints[2]) + fnum(ints[3]))
    row = iota((32, 128), 0)
    col = iota((1, 128), 1)
    i3, i4 = fnum((row >> 2) & 3), fnum(row & 3)
    j2, j3, j4 = fnum((col >> 4) & 3), fnum((col >> 2) & 3), fnum(col & 3)

    def node(k, n):
        return node_energy(fl, k, n) + fl[14 + k] * drive_weight(n)

    ai = t12 * (fl[8] * (i3 * i4) + node(4, i4))
    aj = t12 * (fl[7] * (j2 * j3) + fl[8] * (j3 * j4) + node(3, j3) + node(4, j4))
    mag = jnp.exp(
        -t12 * (fl[12] * ((i3 - j3) * (i3 - j3)) + fl[13] * ((i4 - j4) * (i4 - j4)))
    )
    si, ci = sincos(ai)
    sj, cj = sincos(aj)
    far[...] = mag * (ci * cj + si * sj)
    fai[...] = mag * (ci * sj - si * cj)


def start_of(ints, gathered):
    rows = iota((8, 2), 0)
    kept = jnp.where(rows < ints[5], gathered[...], 0).astype(F32)
    return jnp.sum(jnp.sum(kept, axis=1, keepdims=True), axis=0, keepdims=True)


def drive_phase(fl, k, time):
    phi = time * fl[14 + k]
    turns = jnp.floor(phi * F32(0.5 / math.pi) + F32(0.5))
    return phi - turns * F32(6.28125) - turns * F32(2 * math.pi - 6.28125)


def energy_of(fl, digits):
    total = node_energy(fl, 0, digits[0])
    for k in range(1, TRANSMONS):
        total = total + node_energy(fl, k, digits[k])
    for k in range(TRANSMONS - 1):
        total = total + fl[5 + k] * (digits[k] * digits[k + 1])
    return total


def factor_parts(fl, span, sign, time, row_digits, col_digits):
    phis = [drive_phase(fl, k, time) for k in range(TRANSMONS)]

    def angle(digits):
        total = (F32(0.5) * span) * energy_of(fl, digits)
        drive = phis[0] * drive_weight(digits[0])
        for k in range(1, TRANSMONS):
            drive = drive + phis[k] * drive_weight(digits[k])
        return total + drive if sign > 0 else total - drive

    return sincos(angle(row_digits)), sincos(angle(col_digits))


def decay_of(fl, row_digits, col_digits):
    total = None
    for k in range(TRANSMONS):
        gap = row_digits[k] - col_digits[k]
        part = fl[9 + k] * (gap * gap)
        total = part if total is None else total + part
    return total


def first_factor(ints, fl, gathered):
    span = fnum(ints[2])
    time = start_of(ints, gathered) + F32(0.5) * span
    row = ints[4] * 32 + iota((32, 128), 0)
    col = iota((1, 1024), 1)
    rd = [fnum((row >> (8 - 2 * k)) & 3) for k in range(TRANSMONS)]
    cd = [fnum((col >> (8 - 2 * k)) & 3) for k in range(TRANSMONS)]
    (si, ci), (sj, cj) = factor_parts(fl, span, 1, time, rd, cd)
    wide = [jnp.concatenate([d] * 8, axis=1) for d in rd]
    mag = jnp.exp(F32(-0.5) * span * decay_of(fl, wide, cd))
    si, ci = jnp.concatenate([si] * 8, axis=1), jnp.concatenate([ci] * 8, axis=1)
    return mag * (ci * cj + si * sj), mag * (ci * sj - si * cj)


def to_rows(blocks):
    return jnp.concatenate(
        [
            blocks[:, c * 1024 + a * 256 : c * 1024 + a * 256 + 256]
            for a in range(4)
            for c in range(2)
        ],
        axis=0,
    )


def to_lanes(rows):
    return jnp.concatenate(
        [rows[(2 * a + c) * 32 : (2 * a + c) * 32 + 32, :] for c in range(2) for a in range(4)],
        axis=1,
    )


def mix_top(o0, rows, transposed):
    out = []
    for a in range(4):
        total = None
        for b in range(4):
            n = 4 * b + a if transposed else 4 * a + b
            part = rows[64 * b : 64 * b + 64, :] * o0[n : n + 1, :]
            total = part if total is None else total + part
        out.append(total)
    return jnp.concatenate(out, axis=0)


def chunk_of_lane(shape):
    return (iota(shape, 1) >> 5) & 3


def send(out, offset, x):
    for c in range(2):
        for half in range(2):
            tiles = [
                x[:, c * 1024 + a * 256 + half * 128 : c * 1024 + a * 256 + half * 128 + 128]
                for a in range(4)
            ]
            chunk = chunk_of_lane((32, 128))
            for q in range(4):
                moved = [
                    tiles[a] if a == q else pltpu.roll(tiles[a], ((a - q) * 32) % 128, 1)
                    for a in range(4)
                ]
                merged = pick(chunk, moved)
                for i4 in range(4):
                    out[i4 * 8 + half * 4 + q, :, offset + c * 128 : offset + c * 128 + 128] = (
                        merged[i4 * 8 : i4 * 8 + 8, :]
                    )


def receive(ref, offset):
    chunk = chunk_of_lane((32, 128))
    pieces = {}
    for c in range(2):
        for half in range(2):
            merged = [
                jnp.concatenate(
                    [
                        ref[i4 * 8 + half * 4 + q, :, offset + c * 128 : offset + c * 128 + 128]
                        for i4 in range(4)
                    ],
                    axis=0,
                )
                for q in range(4)
            ]
            for a in range(4):
                moved = [
                    merged[q] if a == q else pltpu.roll(merged[q], ((q - a) * 32) % 128, 1)
                    for q in range(4)
                ]
                pieces[c, a, half] = pick(chunk, moved)
    return jnp.concatenate(
        [pieces[c, a, half] for c in range(2) for a in range(4) for half in range(2)], axis=1
    )


def apply_pointwise_a(rows, far, fai, conj):
    fr = jnp.concatenate([far, far], axis=1)
    fi = jnp.concatenate([fai, fai], axis=1)
    if conj:
        fi = -fi
    out = []
    for a in range(4):
        re, im = rows[64 * a : 64 * a + 32, :], rows[64 * a + 32 : 64 * a + 64, :]
        out += [re * fr - im * fi, re * fi + im * fr]
    return jnp.concatenate(out, axis=0)


def forward_a_kernel(
    ints, fl, gathered, x, f, w1h, w1l, w2h, w2l, wp, r1, r2, far, fai, o0, out
):
    fr, fi = first_factor(ints, fl, gathered)
    re, im = x[0], x[1]
    both = jnp.concatenate([re * fr - im * fi, re * fi + im * fr], axis=1)
    both = left(r1[0], r1[1], both)
    rows = mix_top(o0, to_rows(both), False)
    rows = mm(rows, w1h[...], w1l[...])
    rows = apply_pointwise_a(rows, far[...], fai[...], False)
    rows = mm(rows, w2h[...], w2l[...])
    send(out, 0, left(r2[0], r2[1], to_lanes(rows)))
    rows = to_rows(jnp.concatenate([f[0], f[1]], axis=1))
    send(out, 256, pleft(r2[4], to_lanes(pmm(rows, wp[...]))))


def adjoint_a_kernel(
    ints, fl, gathered, y, m, w1h, w1l, w2h, w2l, wp, r1, r2, far, fai, o0, out
):
    rows = to_rows(left(r2[2], r2[3], receive(y, 0)))
    rows = mm(rows, w2h[...], w2l[...], True)
    rows = apply_pointwise_a(rows, far[...], fai[...], True)
    rows = mm(rows, w1h[...], w1l[...], True)
    rows = mix_top(o0, rows, True)
    both = left(r1[2], r1[3], to_lanes(rows))
    fr, fi = first_factor(ints, fl, gathered)
    re, im = both[:, :1024], both[:, 1024:]
    other = to_lanes(pmm(to_rows(pleft(r2[6], receive(m, 0))), wp[...], True))
    out[0] = re * fr + im * fi - other[:, :1024]
    out[1] = im * fr - re * fi - other[:, 1024:]


def table_b_kernel(
    ints, fl, gathered, pulse, a1h, a1l, b1h, b1l, a2h, a2l, b2h, b2l, vh, vl, fmr, fmi, ffr, ffi
):
    w = 256
    lane = iota((1, w), 1)
    natural = [(lane >> 6) & 3, (lane >> 4) & 3, (lane >> 2) & 3, lane & 3]
    eye = identity(w)
    first = [rotation(ints, pulse, 0, k, w) for k in range(3)]
    second = [rotation(ints, pulse, 1, k, w) for k in range(4)]
    store_kron(a1h, a1l, [*first, eye], natural)
    store_kron(b1h, b1l, [*(flip(o) for o in first), eye], natural)
    store_kron(a2h, a2l, second, natural)
    store_kron(b2h, b2l, [flip(o) for o in second], natural)
    row = iota((16, w), 0)
    cl, l0, l1, l2, ll = (lane >> 7), (lane >> 5) & 3, (lane >> 3) & 3, (lane >> 1) & 3, lane & 1
    t0 = lane_rows(flip(second[0]), l0)
    t1 = lane_rows(flip(second[1]), l1)
    t2 = lane_rows(flip(second[2]), l2)
    low = pick((row >> 1) & 3, t2) * jnp.where((row & 1) == ll, F32(1.0), F32(0.0))
    high_bit = row >> 3
    for n in range(16):
        c, d0, top = n >> 3, (n >> 1) & 3, n & 1
        mid = jnp.where(high_bit == 0, t1[2 * top], t1[2 * top + 1])
        block = low * mid * (t0[d0] * jnp.where(cl == c, F32(1.0), F32(0.0)))
        hi, lo = split(block)
        vh[16 * n : 16 * n + 16, :] = hi
        vl[16 * n : 16 * n + 16, :] = lo
    row = iota((256, 128), 0)
    col = iota((1, 128), 1)
    rd = [fnum((row >> (6 - 2 * k)) & 3) for k in range(4)]
    cd = [fnum((col >> 5) & 3), fnum((col >> 3) & 3), fnum((col >> 1) & 3)]
    t12 = F32(0.5) * (fnum(ints[2]) + fnum(ints[3]))

    def node(k, n):
        return node_energy(fl, k, n) + fl[14 + k] * drive_weight(n)

    ai = fl[5] * (rd[0] * rd[1]) + fl[6] * (rd[1] * rd[2]) + fl[7] * (rd[2] * rd[3])
    for k in range(4):
        ai = ai + node(k, rd[k])
    aj = fl[5] * (cd[0] * cd[1]) + fl[6] * (cd[1] * cd[2])
    for k in range(3):
        aj = aj + node(k, cd[k])
    gap = None
    for k in range(3):
        part = fl[9 + k] * ((rd[k] - cd[k]) * (rd[k] - cd[k]))
        gap = part if gap is None else gap + part
    mag = jnp.exp(-t12 * gap)
    si, ci = sincos(t12 * ai)
    sj, cj = sincos(t12 * aj)
    fmr[...] = mag * (ci * cj + si * sj)
    fmi[...] = mag * (ci * sj - si * cj)
    rank = ints[4]
    i4 = fnum(jnp.full((256, 128), rank >> 3, jnp.int32))
    j3 = fnum(jnp.full((1, 128), (rank >> 1) & 3, jnp.int32))
    j4 = fnum((rank & 1) * 2 + (col & 1))
    rows = [*rd, i4]
    cols = [*cd, j3, j4]
    span = fnum(ints[3])
    time = start_of(ints, gathered) + (fnum(ints[2]) + F32(0.5) * span)
    (si, ci), (sj, cj) = factor_parts(fl, span, -1, time, rows, cols)
    mag = jnp.exp(F32(-0.5) * span * decay_of(fl, rows, cols))
    ffr[...] = mag * (ci * cj + si * sj)
    ffi[...] = mag * (ci * sj - si * cj)


def cmul(x, fr, fi, conj=False):
    re, im = x[:, :128], x[:, 128:]
    if conj:
        return jnp.concatenate([re * fr + im * fi, im * fr - re * fi], axis=1)
    return jnp.concatenate([re * fr - im * fi, re * fi + im * fr], axis=1)


def both_b_kernel(x, a1h, a1l, b1h, b1l, a2h, a2l, b2h, b2l, vh, vl, fmr, fmi, ffr, ffi, out):
    z = left(a1h[...], a1l[...], x[:, :256])
    z = cmul(z, fmr[...], fmi[...])
    z = left(a2h[...], a2l[...], z)
    z = mm(z, vh[...], vl[...])
    z = cmul(z, ffr[...], ffi[...]) - x[:, 256:]
    out[:, 256:] = z
    z = cmul(z, ffr[...], ffi[...], True)
    z = left(b2h[...], b2l[...], z)
    z = mm(z, vh[...], vl[...], True)
    z = cmul(z, fmr[...], fmi[...], True)
    out[:, :256] = left(b1h[...], b1l[...], z)


SMEM = pl.BlockSpec(memory_space=pltpu.SMEM)
VMEM = pl.BlockSpec(memory_space=pltpu.VMEM)


def call(kernel, args, scalars, outs, flops, name):
    specs = [SMEM if n in scalars else VMEM for n in range(len(args))]
    return pl.pallas_call(
        kernel,
        in_specs=specs,
        out_specs=jax.tree.map(lambda _: VMEM, outs),
        out_shape=outs,
        name=name,
        compiler_params=pltpu.CompilerParams(vmem_limit_bytes=16 << 20),
        cost_estimate=pl.CostEstimate(flops=flops, transcendentals=0, bytes_accessed=1 << 20),
    )(*args)


def sds(*shape, dtype=F32):
    return jax.ShapeDtypeStruct(shape, dtype)


def local(linkage, pulse, segments, ticks, detuning, level_shift, coupling, dephase):
    current = linkage[:, 0]
    phases = lax.axis_size("phase")
    ints = jnp.concatenate(
        [
            segments[0],
            ticks[0],
            jnp.stack([lax.axis_index("row"), lax.axis_index("phase")]).astype(jnp.int32),
        ]
    )
    floats = jnp.concatenate([level_shift, coupling, dephase, detuning])
    flat_pulse = pulse.reshape(-1)
    gathered = lax.all_to_all(
        jnp.broadcast_to(ticks, (phases, STEPS)), "phase", split_axis=0, concat_axis=0, tiled=True
    )
    following = lax.ppermute(
        current, "phase", [((i + 1) % phases, i) for i in range(phases)]
    )
    square = sds(256, 256, dtype=BF16)
    tables_a = call(
        table_a_kernel,
        (ints, floats, flat_pulse),
        (0, 1, 2),
        (
            *([square] * 5),
            sds(4, 32, 32, dtype=BF16),
            sds(8, 32, 32, dtype=BF16),
            sds(32, 128),
            sds(32, 128),
            sds(16, 256),
        ),
        1 << 28,
        "table_a",
    )
    sent = call(
        forward_a_kernel,
        (ints, floats, gathered, current, following, *tables_a),
        (0, 1),
        sds(32, 8, 512),
        1 << 28,
        "forward_a",
    )
    turned = lax.all_to_all(sent, "row", split_axis=0, concat_axis=0, tiled=True)
    tables_b = call(
        table_b_kernel,
        (ints, floats, gathered, flat_pulse),
        (0, 1, 3),
        (*([square] * 10), *([sds(256, 128)] * 4)),
        1 << 30,
        "table_b",
    )
    back = call(
        both_b_kernel,
        (turned.reshape(256, 512), *tables_b),
        (),
        sds(256, 512),
        1 << 28,
        "both_b",
    )
    returned = lax.all_to_all(
        back.reshape(32, 8, 512), "row", split_axis=0, concat_axis=0, tiled=True
    )
    earlier = lax.ppermute(
        returned[:, :, 256:], "phase", [(i, (i + 1) % phases) for i in range(phases)]
    )
    result = call(
        adjoint_a_kernel,
        (ints, floats, gathered, returned, earlier, *tables_a),
        (0, 1),
        sds(2, 32, 1024),
        1 << 28,
        "adjoint_a",
    )
    return result[:, None]


def solution(mesh):
    return jax.shard_map(
        local,
        mesh=mesh,
        in_specs=(
            P(None, "phase", "row", None),
            P(),
            P("phase", None),
            P("phase", None),
            P(),
            P(),
            P(),
            P(),
        ),
        out_specs=P(None, "phase", "row", None),
        check_vma=False,
    )
```

```python
import math

import jax
import jax.numpy as jnp
from jax import lax
from jax.experimental import pallas as pl
from jax.experimental.pallas import tpu as pltpu
from jax.sharding import PartitionSpec as P

TRANSMONS = 5
LEVELS = 4
STEPS = 2


F32 = jnp.float32
BF16 = jnp.bfloat16


def iota(shape, dim):
    return lax.broadcasted_iota(jnp.int32, shape, dim)


def sincos(x):
    q = jnp.floor(x * F32(2.0 / math.pi) + F32(0.5))
    r = x - q * F32(1.5703125)
    r = r - q * F32(4.837512969970703125e-4)
    r = r - q * F32(7.549789948768648e-8)
    z = r * r
    s = r + r * z * (F32(-1 / 6) + z * (F32(1 / 120) + z * (F32(-1 / 5040) + z * F32(1 / 362880))))
    c = F32(1.0) + z * (
        F32(-0.5) + z * (F32(1 / 24) + z * (F32(-1 / 720) + z * F32(1 / 40320)))
    )
    k = q.astype(jnp.int32)
    odd = (k & 1) == 1
    sin = jnp.where(odd, c, s)
    cos = jnp.where(odd, s, c)
    sin = jnp.where((k & 2) == 2, -sin, sin)
    cos = jnp.where(((k + 1) & 2) == 2, -cos, cos)
    return sin, cos


def split(x):
    hi = x.astype(BF16)
    return hi, (x - hi.astype(F32)).astype(BF16)


def dot(a, b, transposed=False):
    dims = (((1,), (1 if transposed else 0,)), ((), ()))
    return lax.dot_general(a, b, dims, preferred_element_type=F32)


def mm(x, hi, lo, transposed=False):
    a, b = split(x)
    return dot(a, hi, transposed) + dot(a, lo, transposed) + dot(b, hi, transposed)


def left(hi, lo, x):
    a, b = split(x)
    return dot(hi, a) + dot(hi, b) + dot(lo, a)


def pmm(x, w, transposed=False):
    a, b = split(x)
    return dot(a, w, transposed) + dot(b, w, transposed)


def pleft(w, x):
    a, b = split(x)
    return dot(w, a) + dot(w, b)


def rotation(ints, pulse, step, k, width):
    sc = [sincos(jnp.full((1, width), pulse[k, m, ints[step]], F32)) for m in range(3)]
    (s0, c0), (s1, c1), (s2, c2) = sc
    zero = jnp.zeros((1, width), F32)
    return [
        [c0, -s0 * c1, s0 * s1 * c2, -s0 * s1 * s2],
        [s0, c0 * c1, -c0 * s1 * c2, c0 * s1 * s2],
        [zero, s1, c1 * c2, -c1 * s2],
        [zero, zero, s2, c2],
    ]


def identity(width):
    one, zero = jnp.ones((1, width), F32), jnp.zeros((1, width), F32)
    return [[one if a == b else zero for b in range(4)] for a in range(4)]


def flip(o):
    return [[o[b][a] for b in range(4)] for a in range(4)]


def pick(digit, choices):
    out = choices[3]
    for v in (2, 1, 0):
        out = jnp.where(digit == v, choices[v], out)
    return out


def lane_rows(o, lane_digit):
    return [pick(lane_digit, o[x]) for x in range(4)]


def kron_blocks(mats, lane_digits):
    width = lane_digits[0].shape[1]
    t = [lane_rows(o, d) for o, d in zip(mats, lane_digits)]
    row = iota((16, width), 0)
    low = pick(row >> 2, t[2]) * pick(row & 3, t[3])
    return [low * (t[0][a] * t[1][b]) for a in range(4) for b in range(4)]


def store_kron(hi_ref, lo_ref, mats, lane_digits):
    for n, block in enumerate(kron_blocks(mats, lane_digits)):
        hi, lo = split(block)
        hi_ref[16 * n : 16 * n + 16, :] = hi
        lo_ref[16 * n : 16 * n + 16, :] = lo


def small_table(row_digits, lane_digits, mats):
    out = None
    for o, rd, ld in zip(mats, row_digits, lane_digits):
        part = pick(rd, lane_rows(o, ld))
        out = part if out is None else out * part
    return out


def fnum(x):
    return x.astype(F32)


def node_energy(fl, k, n):
    return fl[k] * (n * (n - F32(1.0)) * F32(0.5))


def drive_weight(n):
    return n * (n + F32(1.0)) * F32(0.5)


def moved_lanes(lane):
    return [
        (lane >> 3) & 3,
        (lane >> 1) & 3,
        (lane >> 6) & 3,
        ((lane >> 5) & 1) * 2 + (lane & 1),
    ]


def lane_moves():
    j1, j2, j3, j4 = moved_lanes(iota((1, 256), 1))
    lanes = iota((256, 256), 0) == j1 * 64 + j2 * 16 + j3 * 4 + j4
    return jnp.where(lanes, F32(1.0), F32(0.0)).astype(BF16)


def row_moves(back):
    n = iota((32, 32), 0 if back else 1)
    m = iota((32, 32), 1 if back else 0)
    rows = n == ((m >> 2) & 1) * 16 + (m & 3) * 4 + (m >> 3)
    return jnp.where(rows, F32(1.0), F32(0.0)).astype(BF16)


def table_a_kernel(ints, fl, pulse, x, w1h, w1l, w2h, w2l, r1, r2, far, fai, o0, gx, gr, gi):
    w = 256
    lane = iota((1, w), 1)
    natural = [(lane >> 6) & 3, (lane >> 4) & 3, (lane >> 2) & 3, lane & 3]
    moved = moved_lanes(lane)
    eye = identity(w)
    first = [rotation(ints, pulse, 0, k, w) for k in range(TRANSMONS)]
    second = {k: rotation(ints, pulse, 1, k, w) for k in (3, 4)}
    store_kron(w1h, w1l, [flip(first[k]) for k in (1, 2, 3, 4)], natural)
    store_kron(w2h, w2l, [eye, eye, flip(second[3]), flip(second[4])], moved)
    for a in range(4):
        for b in range(4):
            o0[4 * a + b : 4 * a + b + 1, :] = first[0][a][b]
    rl = iota((1, 32), 1)
    rr = iota((32, 32), 0)
    one = [[e[:, :32] for e in row] for row in eye]
    f3 = [[e[:, :32] for e in row] for row in first[3]]
    f4 = [[e[:, :32] for e in row] for row in first[4]]
    g4 = [[e[:, :32] for e in row] for row in second[4]]
    nat_r = [rr >> 4, (rr >> 2) & 3, rr & 3]
    nat_l = [rl >> 4, (rl >> 2) & 3, rl & 3]
    mov_r = [(rr >> 2) & 1, rr & 3, rr >> 3]
    mov_l = [(rl >> 2) & 1, rl & 3, rl >> 3]
    tables = [
        small_table(nat_r, nat_l, [one, f3, f4]),
        small_table(nat_r, nat_l, [one, flip(f3), flip(f4)]),
    ]
    for n, t in enumerate(tables):
        hi, lo = split(t)
        r1[2 * n], r1[2 * n + 1] = hi, lo
    tables = [
        small_table(mov_r, nat_l, [one, one, g4]),
        small_table(nat_r, mov_l, [one, one, flip(g4)]),
    ]
    for n, t in enumerate(tables):
        hi, lo = split(t)
        r2[2 * n], r2[2 * n + 1] = hi, lo
    t12 = F32(0.5) * (fnum(ints[2]) + fnum(ints[3]))
    row = iota((32, 128), 0)
    col = iota((1, 128), 1)
    i3, i4 = fnum((row >> 2) & 3), fnum(row & 3)
    j2, j3, j4 = fnum((col >> 4) & 3), fnum((col >> 2) & 3), fnum(col & 3)

    def node(k, n):
        return node_energy(fl, k, n) + fl[14 + k] * drive_weight(n)

    ai = t12 * (fl[8] * (i3 * i4) + node(4, i4))
    aj = t12 * (fl[7] * (j2 * j3) + fl[8] * (j3 * j4) + node(3, j3) + node(4, j4))
    mag = jnp.exp(
        -t12 * (fl[12] * ((i3 - j3) * (i3 - j3)) + fl[13] * ((i4 - j4) * (i4 - j4)))
    )
    si, ci = sincos(ai)
    sj, cj = sincos(aj)
    far[...] = mag * (ci * cj + si * sj)
    fai[...] = mag * (ci * sj - si * cj)
    span = fnum(ints[2])
    rd, cd = digits_a(ints)
    (si, ci), (sj, cj) = factor_parts(fl, span, 1, F32(0.5) * span, rd, cd)
    wide = [jnp.concatenate([d] * 8, axis=1) for d in rd]
    mag = jnp.exp(F32(-0.5) * span * decay_of(fl, wide, cd))
    si, ci = jnp.concatenate([si] * 8, axis=1), jnp.concatenate([ci] * 8, axis=1)
    fr, fi = mag * (ci * cj + si * sj), mag * (ci * sj - si * cj)
    gr[...] = fr
    gi[...] = fi
    re, im = x[0], x[1]
    gx[0] = re * fr - im * fi
    gx[1] = re * fi + im * fr


def digits_a(ints):
    row = ints[4] * 32 + iota((32, 128), 0)
    col = iota((1, 1024), 1)
    rd = [fnum((row >> (8 - 2 * k)) & 3) for k in range(TRANSMONS)]
    cd = [fnum((col >> (8 - 2 * k)) & 3) for k in range(TRANSMONS)]
    return rd, cd


def start_of(ints, gathered):
    rows = iota((8, 2), 0)
    kept = jnp.where(rows < ints[5], gathered[...], 0).astype(F32)
    return jnp.sum(jnp.sum(kept, axis=1, keepdims=True), axis=0, keepdims=True)


def drive_phase(fl, k, time):
    phi = time * fl[14 + k]
    turns = jnp.floor(phi * F32(0.5 / math.pi) + F32(0.5))
    return phi - turns * F32(6.28125) - turns * F32(2 * math.pi - 6.28125)


def energy_of(fl, digits):
    total = node_energy(fl, 0, digits[0])
    for k in range(1, TRANSMONS):
        total = total + node_energy(fl, k, digits[k])
    for k in range(TRANSMONS - 1):
        total = total + fl[5 + k] * (digits[k] * digits[k + 1])
    return total


def factor_parts(fl, span, sign, time, row_digits, col_digits):
    phis = [drive_phase(fl, k, time) for k in range(TRANSMONS)]

    def angle(digits):
        total = (F32(0.5) * span) * energy_of(fl, digits)
        drive = phis[0] * drive_weight(digits[0])
        for k in range(1, TRANSMONS):
            drive = drive + phis[k] * drive_weight(digits[k])
        return total + drive if sign > 0 else total - drive

    return sincos(angle(row_digits)), sincos(angle(col_digits))


def decay_of(fl, row_digits, col_digits):
    total = None
    for k in range(TRANSMONS):
        gap = row_digits[k] - col_digits[k]
        part = fl[9 + k] * (gap * gap)
        total = part if total is None else total + part
    return total


def start_factor(ints, fl, gathered):
    time = start_of(ints, gathered)
    rd, cd = digits_a(ints)
    phis = [drive_phase(fl, k, time) for k in range(TRANSMONS)]

    def angle(digits):
        total = phis[0] * drive_weight(digits[0])
        for k in range(1, TRANSMONS):
            total = total + phis[k] * drive_weight(digits[k])
        return total

    si, ci = sincos(angle(rd))
    sj, cj = sincos(angle(cd))
    si, ci = jnp.concatenate([si] * 8, axis=1), jnp.concatenate([ci] * 8, axis=1)
    return ci * cj + si * sj, ci * sj - si * cj


def to_rows(blocks):
    return jnp.concatenate(
        [
            blocks[:, c * 1024 + a * 256 : c * 1024 + a * 256 + 256]
            for a in range(4)
            for c in range(2)
        ],
        axis=0,
    )


def to_lanes(rows):
    return jnp.concatenate(
        [rows[(2 * a + c) * 32 : (2 * a + c) * 32 + 32, :] for c in range(2) for a in range(4)],
        axis=1,
    )


def mix_top(o0, rows, transposed):
    out = []
    for a in range(4):
        total = None
        for b in range(4):
            n = 4 * b + a if transposed else 4 * a + b
            part = rows[64 * b : 64 * b + 64, :] * o0[n : n + 1, :]
            total = part if total is None else total + part
        out.append(total)
    return jnp.concatenate(out, axis=0)


def chunk_of_lane(shape):
    return (iota(shape, 1) >> 5) & 3


def send(out, offset, x):
    for c in range(2):
        for half in range(2):
            tiles = [
                x[:, c * 1024 + a * 256 + half * 128 : c * 1024 + a * 256 + half * 128 + 128]
                for a in range(4)
            ]
            chunk = chunk_of_lane((32, 128))
            for q in range(4):
                moved = [
                    tiles[a] if a == q else pltpu.roll(tiles[a], ((a - q) * 32) % 128, 1)
                    for a in range(4)
                ]
                merged = pick(chunk, moved)
                for i4 in range(4):
                    out[i4 * 8 + half * 4 + q, :, offset + c * 128 : offset + c * 128 + 128] = (
                        merged[i4 * 8 : i4 * 8 + 8, :]
                    )


def receive(ref, offset):
    chunk = chunk_of_lane((32, 128))
    pieces = {}
    for c in range(2):
        for half in range(2):
            merged = [
                jnp.concatenate(
                    [
                        ref[i4 * 8 + half * 4 + q, :, offset + c * 128 : offset + c * 128 + 128]
                        for i4 in range(4)
                    ],
                    axis=0,
                )
                for q in range(4)
            ]
            for a in range(4):
                moved = [
                    merged[q] if a == q else pltpu.roll(merged[q], ((q - a) * 32) % 128, 1)
                    for q in range(4)
                ]
                pieces[c, a, half] = pick(chunk, moved)
    return jnp.concatenate(
        [pieces[c, a, half] for c in range(2) for a in range(4) for half in range(2)], axis=1
    )


def apply_pointwise_a(rows, far, fai, conj):
    fr = jnp.concatenate([far, far], axis=1)
    fi = jnp.concatenate([fai, fai], axis=1)
    if conj:
        fi = -fi
    out = []
    for a in range(4):
        re, im = rows[64 * a : 64 * a + 32, :], rows[64 * a + 32 : 64 * a + 64, :]
        out += [re * fr - im * fi, re * fi + im * fr]
    return jnp.concatenate(out, axis=0)


def raw_kernel(x, out):
    blocks = to_rows(jnp.concatenate([x[0], x[1]], axis=1))
    send(out, 0, pleft(row_moves(False), to_lanes(pmm(blocks, lane_moves()))))


def forward_a_kernel(
    ints, fl, gathered, gx, other, w1h, w1l, w2h, w2l, r1, r2, far, fai, o0, out
):
    out[:, :, 256:] = other[...]
    fr, fi = start_factor(ints, fl, gathered)
    re, im = gx[0], gx[1]
    both = jnp.concatenate([re * fr - im * fi, re * fi + im * fr], axis=1)
    both = left(r1[0], r1[1], both)
    rows = mix_top(o0, to_rows(both), False)
    rows = mm(rows, w1h[...], w1l[...])
    rows = apply_pointwise_a(rows, far[...], fai[...], False)
    rows = mm(rows, w2h[...], w2l[...])
    send(out, 0, left(r2[0], r2[1], to_lanes(rows)))


def adjoint_a_kernel(
    ints, fl, gathered, y, w1h, w1l, w2h, w2l, r1, r2, far, fai, o0, gr, gi, out
):
    rows = to_rows(left(r2[2], r2[3], receive(y, 0)))
    rows = mm(rows, w2h[...], w2l[...], True)
    rows = apply_pointwise_a(rows, far[...], fai[...], True)
    rows = mm(rows, w1h[...], w1l[...], True)
    rows = mix_top(o0, rows, True)
    both = left(r1[2], r1[3], to_lanes(rows))
    sr, si = start_factor(ints, fl, gathered)
    fr, fi = gr[...] * sr - gi[...] * si, gr[...] * si + gi[...] * sr
    re, im = both[:, :1024], both[:, 1024:]
    out[0] = re * fr + im * fi
    out[1] = im * fr - re * fi


def finish_kernel(x, m, out):
    rows = to_rows(pleft(row_moves(True), receive(m, 0)))
    other = to_lanes(pmm(rows, lane_moves(), True))
    out[0] = x[0] - other[:, :1024]
    out[1] = x[1] - other[:, 1024:]


def table_b_kernel(
    ints, fl, pulse, gathered, a1h, a1l, b1h, b1l, a2h, a2l, b2h, b2l, vh, vl, fmr, fmi, ffr, ffi
):
    w = 256
    lane = iota((1, w), 1)
    natural = [(lane >> 6) & 3, (lane >> 4) & 3, (lane >> 2) & 3, lane & 3]
    eye = identity(w)
    first = [rotation(ints, pulse, 0, k, w) for k in range(3)]
    second = [rotation(ints, pulse, 1, k, w) for k in range(4)]
    store_kron(a1h, a1l, [*first, eye], natural)
    store_kron(b1h, b1l, [*(flip(o) for o in first), eye], natural)
    store_kron(a2h, a2l, second, natural)
    store_kron(b2h, b2l, [flip(o) for o in second], natural)
    row = iota((16, w), 0)
    cl, l0, l1, l2, ll = (lane >> 7), (lane >> 5) & 3, (lane >> 3) & 3, (lane >> 1) & 3, lane & 1
    t0 = lane_rows(flip(second[0]), l0)
    t1 = lane_rows(flip(second[1]), l1)
    t2 = lane_rows(flip(second[2]), l2)
    low = pick((row >> 1) & 3, t2) * jnp.where((row & 1) == ll, F32(1.0), F32(0.0))
    high_bit = row >> 3
    for n in range(16):
        c, d0, top = n >> 3, (n >> 1) & 3, n & 1
        mid = jnp.where(high_bit == 0, t1[2 * top], t1[2 * top + 1])
        block = low * mid * (t0[d0] * jnp.where(cl == c, F32(1.0), F32(0.0)))
        hi, lo = split(block)
        vh[16 * n : 16 * n + 16, :] = hi
        vl[16 * n : 16 * n + 16, :] = lo
    row = iota((256, 128), 0)
    col = iota((1, 128), 1)
    rd = [fnum((row >> (6 - 2 * k)) & 3) for k in range(4)]
    cd = [fnum((col >> 5) & 3), fnum((col >> 3) & 3), fnum((col >> 1) & 3)]
    t12 = F32(0.5) * (fnum(ints[2]) + fnum(ints[3]))

    def node(k, n):
        return node_energy(fl, k, n) + fl[14 + k] * drive_weight(n)

    ai = fl[5] * (rd[0] * rd[1]) + fl[6] * (rd[1] * rd[2]) + fl[7] * (rd[2] * rd[3])
    for k in range(4):
        ai = ai + node(k, rd[k])
    aj = fl[5] * (cd[0] * cd[1]) + fl[6] * (cd[1] * cd[2])
    for k in range(3):
        aj = aj + node(k, cd[k])
    gap = None
    for k in range(3):
        part = fl[9 + k] * ((rd[k] - cd[k]) * (rd[k] - cd[k]))
        gap = part if gap is None else gap + part
    mag = jnp.exp(-t12 * gap)
    si, ci = sincos(t12 * ai)
    sj, cj = sincos(t12 * aj)
    fmr[...] = mag * (ci * cj + si * sj)
    fmi[...] = mag * (ci * sj - si * cj)
    rank = ints[4]
    i4 = fnum(jnp.full((256, 128), rank >> 3, jnp.int32))
    j3 = fnum(jnp.full((1, 128), (rank >> 1) & 3, jnp.int32))
    j4 = fnum((rank & 1) * 2 + (col & 1))
    rows = [*rd, i4]
    cols = [*cd, j3, j4]
    span = fnum(ints[3])
    time = start_of(ints, gathered) + (fnum(ints[2]) + F32(0.5) * span)
    (si, ci), (sj, cj) = factor_parts(fl, span, -1, time, rows, cols)
    mag = jnp.exp(F32(-0.5) * span * decay_of(fl, rows, cols))
    ffr[...] = mag * (ci * cj + si * sj)
    ffi[...] = mag * (ci * sj - si * cj)


def cmul(x, fr, fi, conj=False):
    re, im = x[:, :128], x[:, 128:]
    if conj:
        return jnp.concatenate([re * fr + im * fi, im * fr - re * fi], axis=1)
    return jnp.concatenate([re * fr - im * fi, re * fi + im * fr], axis=1)


def both_b_kernel(x, a1h, a1l, b1h, b1l, a2h, a2l, b2h, b2l, vh, vl, fmr, fmi, ffr, ffi, out):
    z = left(a1h[...], a1l[...], x[:, :256])
    z = cmul(z, fmr[...], fmi[...])
    z = left(a2h[...], a2l[...], z)
    z = mm(z, vh[...], vl[...])
    z = cmul(z, ffr[...], ffi[...]) - x[:, 256:]
    out[:, 256:] = z
    z = cmul(z, ffr[...], ffi[...], True)
    z = left(b2h[...], b2l[...], z)
    z = mm(z, vh[...], vl[...], True)
    z = cmul(z, fmr[...], fmi[...], True)
    out[:, :256] = left(b1h[...], b1l[...], z)


SMEM = pl.BlockSpec(memory_space=pltpu.SMEM)
VMEM = pl.BlockSpec(memory_space=pltpu.VMEM)


def with_params(kernel):
    def run(segment, tick, rank, shift, coupling, dephase, detuning, *refs):
        ints = [segment[0, 0], segment[0, 1], tick[0, 0], tick[0, 1], rank[0], rank[1]]
        sources = ((shift, 5), (coupling, 4), (dephase, 5), (detuning, 5))
        kernel(ints, [ref[n] for ref, count in sources for n in range(count)], *refs)

    return run


def call(kernel, args, scalars, outs, flops, name):
    specs = [SMEM if n < scalars else VMEM for n in range(len(args))]
    return pl.pallas_call(
        with_params(kernel) if scalars else kernel,
        in_specs=specs,
        out_specs=jax.tree.map(lambda _: VMEM, outs),
        out_shape=outs,
        name=name,
        compiler_params=pltpu.CompilerParams(vmem_limit_bytes=16 << 20),
        cost_estimate=pl.CostEstimate(flops=flops, transcendentals=0, bytes_accessed=1 << 20),
    )(*args)


def sds(*shape, dtype=F32):
    return jax.ShapeDtypeStruct(shape, dtype)


def local(linkage, pulse, segments, ticks, detuning, level_shift, coupling, dephase):
    current = linkage[:, 0]
    phases = lax.axis_size("phase")
    rank = jnp.stack([lax.axis_index("row"), lax.axis_index("phase")]).astype(jnp.int32)
    params = (segments, ticks, rank, level_shift, coupling, dephase, detuning)
    angles = jnp.transpose(pulse, (1, 2, 0))
    gathered = lax.all_to_all(
        jnp.broadcast_to(ticks, (phases, STEPS)), "phase", split_axis=0, concat_axis=0, tiled=True
    )
    def turn(x):
        return lax.all_to_all(
            x.reshape(32, 8, 512), "row", split_axis=0, concat_axis=0, tiled=True
        )

    following = lax.ppermute(current, "phase", [((i + 1) % phases, i) for i in range(phases)])
    following = call(raw_kernel, (following,), 0, sds(32, 8, 256), 1 << 26, "raw")
    square = sds(256, 256, dtype=BF16)
    *tables_a, weighed, gr, gi = call(
        table_a_kernel,
        (*params, angles, current),
        8,
        (
            *([square] * 4),
            sds(4, 32, 32, dtype=BF16),
            sds(4, 32, 32, dtype=BF16),
            sds(32, 128),
            sds(32, 128),
            sds(16, 256),
            sds(2, 32, 1024),
            sds(32, 1024),
            sds(32, 1024),
        ),
        1 << 28,
        "table_a",
    )
    sent = call(
        forward_a_kernel,
        (*params, gathered, weighed, following, *tables_a),
        7,
        sds(32, 8, 512),
        1 << 28,
        "forward_a",
    )
    turned = turn(sent)
    tables_b = call(
        table_b_kernel,
        (*params, angles, gathered),
        8,
        (*([square] * 10), *([sds(256, 128)] * 4)),
        1 << 28,
        "table_b",
    )
    back = call(
        both_b_kernel,
        (turned.reshape(256, 512), *tables_b),
        0,
        sds(256, 512),
        1 << 28,
        "both_b",
    )
    returned = turn(back)
    earlier = lax.ppermute(
        returned[:, :, 256:], "phase", [(i, (i + 1) % phases) for i in range(phases)]
    )
    costate = call(
        adjoint_a_kernel,
        (*params, gathered, returned, *tables_a, gr, gi),
        7,
        sds(2, 32, 1024),
        1 << 28,
        "adjoint_a",
    )
    result = call(finish_kernel, (costate, earlier), 0, sds(2, 32, 1024), 1 << 26, "finish")
    return result[:, None]


def solution(mesh):
    return jax.shard_map(
        local,
        mesh=mesh,
        in_specs=(
            P(None, "phase", "row", None),
            P(),
            P("phase", None),
            P("phase", None),
            P(),
            P(),
            P(),
            P(),
        ),
        out_specs=P(None, "phase", "row", None),
        check_vma=False,
    )
```

```python
import math

import jax
import jax.numpy as jnp
from jax import lax
from jax.experimental import pallas as pl
from jax.experimental.pallas import tpu as pltpu
from jax.sharding import PartitionSpec as P

TRANSMONS = 5
LEVELS = 4
STEPS = 2


F32 = jnp.float32
BF16 = jnp.bfloat16


def iota(shape, dim):
    return lax.broadcasted_iota(jnp.int32, shape, dim)


def sincos(x):
    q = jnp.floor(x * F32(2.0 / math.pi) + F32(0.5))
    r = x - q * F32(1.5703125)
    r = r - q * F32(4.837512969970703125e-4)
    r = r - q * F32(7.549789948768648e-8)
    z = r * r
    s = r + r * z * (F32(-1 / 6) + z * (F32(1 / 120) + z * (F32(-1 / 5040) + z * F32(1 / 362880))))
    c = F32(1.0) + z * (
        F32(-0.5) + z * (F32(1 / 24) + z * (F32(-1 / 720) + z * F32(1 / 40320)))
    )
    k = q.astype(jnp.int32)
    odd = (k & 1) == 1
    sin = jnp.where(odd, c, s)
    cos = jnp.where(odd, s, c)
    sin = jnp.where((k & 2) == 2, -sin, sin)
    cos = jnp.where(((k + 1) & 2) == 2, -cos, cos)
    return sin, cos


def split(x):
    hi = x.astype(BF16)
    return hi, (x - hi.astype(F32)).astype(BF16)


def dot(a, b, transposed=False):
    dims = (((1,), (1 if transposed else 0,)), ((), ()))
    return lax.dot_general(a, b, dims, preferred_element_type=F32)


def mm(x, hi, lo, transposed=False):
    a, b = split(x)
    return dot(a, hi, transposed) + dot(a, lo, transposed) + dot(b, hi, transposed)


def left(hi, lo, x):
    a, b = split(x)
    return dot(hi, a) + dot(hi, b) + dot(lo, a)


def pmm(x, w, transposed=False):
    a, b = split(x)
    return dot(a, w, transposed) + dot(b, w, transposed)


def pleft(w, x):
    a, b = split(x)
    return dot(w, a) + dot(w, b)


def rotation(ints, pulse, step, k, width):
    sc = [sincos(jnp.full((1, width), pulse[k, m, ints[step]], F32)) for m in range(3)]
    (s0, c0), (s1, c1), (s2, c2) = sc
    zero = jnp.zeros((1, width), F32)
    return [
        [c0, -s0 * c1, s0 * s1 * c2, -s0 * s1 * s2],
        [s0, c0 * c1, -c0 * s1 * c2, c0 * s1 * s2],
        [zero, s1, c1 * c2, -c1 * s2],
        [zero, zero, s2, c2],
    ]


def identity(width):
    one, zero = jnp.ones((1, width), F32), jnp.zeros((1, width), F32)
    return [[one if a == b else zero for b in range(4)] for a in range(4)]


def flip(o):
    return [[o[b][a] for b in range(4)] for a in range(4)]


def pick(digit, choices):
    out = choices[3]
    for v in (2, 1, 0):
        out = jnp.where(digit == v, choices[v], out)
    return out


def lane_rows(o, lane_digit):
    return [pick(lane_digit, o[x]) for x in range(4)]


def kron_blocks(mats, lane_digits):
    width = lane_digits[0].shape[1]
    t = [lane_rows(o, d) for o, d in zip(mats, lane_digits)]
    row = iota((16, width), 0)
    low = pick(row >> 2, t[2]) * pick(row & 3, t[3])
    return [low * (t[0][a] * t[1][b]) for a in range(4) for b in range(4)]


def store_kron(hi_ref, lo_ref, mats, lane_digits):
    for n, block in enumerate(kron_blocks(mats, lane_digits)):
        hi, lo = split(block)
        hi_ref[16 * n : 16 * n + 16, :] = hi
        lo_ref[16 * n : 16 * n + 16, :] = lo


def fnum(x):
    return x.astype(F32)


def node_energy(fl, k, n):
    return fl[k] * (n * (n - F32(1.0)) * F32(0.5))


def drive_weight(n):
    return n * (n + F32(1.0)) * F32(0.5)


def moved_lanes(lane):
    return [
        (lane >> 3) & 3,
        (lane >> 1) & 3,
        (lane >> 6) & 3,
        ((lane >> 5) & 1) * 2 + (lane & 1),
    ]


def lane_moves():
    j1, j2, j3, j4 = moved_lanes(iota((1, 256), 1))
    lanes = iota((256, 256), 0) == j1 * 64 + j2 * 16 + j3 * 4 + j4
    return jnp.where(lanes, F32(1.0), F32(0.0)).astype(BF16)


def moved_row(m):
    return (m & ~31) + ((m >> 2) & 1) * 16 + (m & 3) * 4 + ((m >> 3) & 3)


def row_moves(back):
    if back:
        rows = iota((256, 256), 0) == moved_row(iota((1, 256), 1))
    else:
        rows = moved_row(iota((256, 1), 0)) == iota((256, 256), 1)
    return jnp.where(rows, F32(1.0), F32(0.0)).astype(BF16)


def store_rows_a(hi_ref, lo_ref, o0, o3, o4):
    lane = iota((1, 256), 1)
    row = iota((16, 256), 0)
    t0, t3, t4 = (
        lane_rows(o, d) for o, d in ((o0, (lane >> 6) & 3), (o3, (lane >> 2) & 3), (o4, lane & 3))
    )
    same = ((row >> 2) & 1) == ((lane >> 4) & 1)
    low = pick(row & 3, t3) * jnp.where(same, F32(1.0), F32(0.0))
    mid = [low * jnp.where((row >> 3) == 0, t4[2 * h], t4[2 * h + 1]) for h in range(2)]
    for n in range(16):
        kept = jnp.where(((lane >> 5) & 1) == ((n >> 1) & 1), F32(1.0), F32(0.0))
        hi, lo = split(mid[n & 1] * (t0[n >> 2] * kept))
        hi_ref[16 * n : 16 * n + 16, :] = hi
        lo_ref[16 * n : 16 * n + 16, :] = lo


def table_a_kernel(
    ints, fl, pulse, source, w1h, w1l, w2h, w2l, k1h, k1l, far, fai, o4, gx, x, sem
):
    fetch = pltpu.make_async_copy(source, x, sem)
    fetch.start()
    w = 256
    lane = iota((1, w), 1)
    natural = [(lane >> 6) & 3, (lane >> 4) & 3, (lane >> 2) & 3, lane & 3]
    moved = moved_lanes(lane)
    eye = identity(w)
    first = [rotation(ints, pulse, 0, k, w) for k in range(TRANSMONS)]
    second = {k: rotation(ints, pulse, 1, k, w) for k in (3, 4)}
    store_kron(w1h, w1l, [flip(first[k]) for k in (1, 2, 3, 4)], natural)
    store_kron(w2h, w2l, [eye, eye, flip(second[3]), flip(second[4])], moved)
    store_rows_a(k1h, k1l, first[0], first[3], first[4])
    for a in range(4):
        for b in range(4):
            o4[4 * a + b : 4 * a + b + 1, :] = second[4][a][b]
    t12 = F32(0.5) * (fnum(ints[2]) + fnum(ints[3]))
    row = iota((32, 128), 0)
    col = iota((1, 128), 1)
    i3, i4 = fnum(row & 3), fnum(row >> 3)
    j2, j3, j4 = fnum((col >> 4) & 3), fnum((col >> 2) & 3), fnum(col & 3)

    def node(k, n):
        return node_energy(fl, k, n) + fl[14 + k] * drive_weight(n)

    ai = t12 * (fl[8] * (i3 * i4) + node(4, i4))
    aj = t12 * (fl[7] * (j2 * j3) + fl[8] * (j3 * j4) + node(3, j3) + node(4, j4))
    mag = jnp.exp(
        -t12 * (fl[12] * ((i3 - j3) * (i3 - j3)) + fl[13] * ((i4 - j4) * (i4 - j4)))
    )
    si, ci = sincos(ai)
    sj, cj = sincos(aj)
    far[...] = mag * (ci * cj + si * sj)
    fai[...] = mag * (ci * sj - si * cj)
    fr, fi = first_factor(ints, fl, F32(0.5) * fnum(ints[2]))
    fetch.wait()
    re, im = x[0], x[1]
    gx[0] = re * fr - im * fi
    gx[1] = re * fi + im * fr


def first_factor(ints, fl, time):
    span = fnum(ints[2])
    rd, cd = digits_a(ints)
    (si, ci), (sj, cj) = factor_parts(fl, span, 1, time, rd, cd)
    wide = [jnp.concatenate([d] * 8, axis=1) for d in rd]
    mag = jnp.exp(F32(-0.5) * span * decay_of(fl, wide, cd))
    si, ci = jnp.concatenate([si] * 8, axis=1), jnp.concatenate([ci] * 8, axis=1)
    return mag * (ci * cj + si * sj), mag * (ci * sj - si * cj)


def digits_a(ints):
    row = ints[4] * 32 + iota((32, 128), 0)
    col = iota((1, 1024), 1)
    rd = [fnum((row >> (8 - 2 * k)) & 3) for k in range(TRANSMONS)]
    cd = [fnum((col >> (8 - 2 * k)) & 3) for k in range(TRANSMONS)]
    return rd, cd


def start_of(ints, gathered):
    rows = iota((8, 2), 0)
    kept = jnp.where(rows < ints[5], gathered[...], 0).astype(F32)
    return jnp.sum(jnp.sum(kept, axis=1, keepdims=True), axis=0, keepdims=True)


def drive_phase(fl, k, time):
    phi = time * fl[14 + k]
    turns = jnp.floor(phi * F32(0.5 / math.pi) + F32(0.5))
    return phi - turns * F32(6.28125) - turns * F32(2 * math.pi - 6.28125)


def energy_of(fl, digits):
    total = node_energy(fl, 0, digits[0])
    for k in range(1, TRANSMONS):
        total = total + node_energy(fl, k, digits[k])
    for k in range(TRANSMONS - 1):
        total = total + fl[5 + k] * (digits[k] * digits[k + 1])
    return total


def factor_parts(fl, span, sign, time, row_digits, col_digits):
    phis = [drive_phase(fl, k, time) for k in range(TRANSMONS)]

    def angle(digits):
        total = (F32(0.5) * span) * energy_of(fl, digits)
        drive = phis[0] * drive_weight(digits[0])
        for k in range(1, TRANSMONS):
            drive = drive + phis[k] * drive_weight(digits[k])
        return total + drive if sign > 0 else total - drive

    return sincos(angle(row_digits)), sincos(angle(col_digits))


def decay_of(fl, row_digits, col_digits):
    total = None
    for k in range(TRANSMONS):
        gap = row_digits[k] - col_digits[k]
        part = fl[9 + k] * (gap * gap)
        total = part if total is None else total + part
    return total


def start_factor(ints, fl, gathered):
    time = start_of(ints, gathered)
    rd, cd = digits_a(ints)
    phis = [drive_phase(fl, k, time) for k in range(TRANSMONS)]

    def angle(digits):
        total = phis[0] * drive_weight(digits[0])
        for k in range(1, TRANSMONS):
            total = total + phis[k] * drive_weight(digits[k])
        return total

    si, ci = sincos(angle(rd))
    sj, cj = sincos(angle(cd))
    si, ci = jnp.concatenate([si] * 8, axis=1), jnp.concatenate([ci] * 8, axis=1)
    return ci * cj + si * sj, ci * sj - si * cj


def to_rows(blocks):
    return jnp.concatenate(
        [
            blocks[:, c * 1024 + a * 256 : c * 1024 + a * 256 + 256]
            for a in range(4)
            for c in range(2)
        ],
        axis=0,
    )


def to_lanes(rows):
    return jnp.concatenate(
        [rows[(2 * a + c) * 32 : (2 * a + c) * 32 + 32, :] for c in range(2) for a in range(4)],
        axis=1,
    )


def mix_i4(o4, rows, transposed):
    parts = [
        jnp.concatenate([rows[32 * n + 8 * b : 32 * n + 8 * b + 8, :] for n in range(8)], axis=0)
        for b in range(4)
    ]
    out = []
    for a in range(4):
        total = None
        for b in range(4):
            n = 4 * b + a if transposed else 4 * a + b
            part = parts[b] * o4[n : n + 1, :]
            total = part if total is None else total + part
        out.append(total)
    return jnp.concatenate(
        [out[a][8 * n : 8 * n + 8, :] for n in range(8) for a in range(4)], axis=0
    )


def chunk_of_lane(shape):
    return (iota(shape, 1) >> 5) & 3


def send(out, offset, x):
    for c in range(2):
        for half in range(2):
            tiles = [
                x[:, c * 1024 + a * 256 + half * 128 : c * 1024 + a * 256 + half * 128 + 128]
                for a in range(4)
            ]
            chunk = chunk_of_lane((32, 128))
            for q in range(4):
                moved = [
                    tiles[a] if a == q else pltpu.roll(tiles[a], ((a - q) * 32) % 128, 1)
                    for a in range(4)
                ]
                merged = pick(chunk, moved)
                for i4 in range(4):
                    out[i4 * 8 + half * 4 + q, :, offset + c * 128 : offset + c * 128 + 128] = (
                        merged[i4 * 8 : i4 * 8 + 8, :]
                    )


def receive(ref, offset):
    chunk = chunk_of_lane((32, 128))
    pieces = {}
    for c in range(2):
        for half in range(2):
            merged = [
                jnp.concatenate(
                    [
                        ref[i4 * 8 + half * 4 + q, :, offset + c * 128 : offset + c * 128 + 128]
                        for i4 in range(4)
                    ],
                    axis=0,
                )
                for q in range(4)
            ]
            for a in range(4):
                moved = [
                    merged[q] if a == q else pltpu.roll(merged[q], ((q - a) * 32) % 128, 1)
                    for q in range(4)
                ]
                pieces[c, a, half] = pick(chunk, moved)
    return jnp.concatenate(
        [pieces[c, a, half] for c in range(2) for a in range(4) for half in range(2)], axis=1
    )


def apply_pointwise_a(rows, far, fai, conj):
    fr = jnp.concatenate([far, far], axis=1)
    fi = jnp.concatenate([fai, fai], axis=1)
    if conj:
        fi = -fi
    out = []
    for a in range(4):
        re, im = rows[64 * a : 64 * a + 32, :], rows[64 * a + 32 : 64 * a + 64, :]
        out += [re * fr - im * fi, re * fi + im * fr]
    return jnp.concatenate(out, axis=0)


def raw_kernel(x, out):
    rows = to_rows(jnp.concatenate([x[0], x[1]], axis=1))
    send(out, 0, to_lanes(pmm(pleft(row_moves(False), rows), lane_moves())))


def forward_a_kernel(
    ints, fl, gathered, gx, other, w1h, w1l, w2h, w2l, k1h, k1l, far, fai, o4, out
):
    out[:, :, 256:] = other[...]
    fr, fi = start_factor(ints, fl, gathered)
    re, im = gx[0], gx[1]
    rows = to_rows(jnp.concatenate([re * fr - im * fi, re * fi + im * fr], axis=1))
    rows = mm(left(k1h[...], k1l[...], rows), w1h[...], w1l[...])
    rows = apply_pointwise_a(rows, far[...], fai[...], False)
    send(out, 0, to_lanes(mm(mix_i4(o4, rows, False), w2h[...], w2l[...])))


def adjoint_a_kernel(
    ints, fl, pulse, gathered, y, w1h, w1l, w2h, w2l, far, fai, o4, out, t1h, t1l
):
    rows = mm(to_rows(receive(y, 0)), w2h[...], w2l[...], True)
    rows = apply_pointwise_a(mix_i4(o4, rows, True), far[...], fai[...], True)
    rows = mm(rows, w1h[...], w1l[...], True)
    lane = iota((1, 256), 1)
    sent = [
        (lane >> 6) & 3,
        ((lane >> 5) & 1) * 2 + ((lane >> 2) & 1),
        lane & 3,
        (lane >> 3) & 3,
    ]
    first = [flip(rotation(ints, pulse, 0, k, 256)) for k in (0, 3, 4)]
    store_kron(t1h, t1l, [first[0], identity(256), first[1], first[2]], sent)
    both = to_lanes(left(t1h[...], t1l[...], rows))
    fr, fi = first_factor(ints, fl, start_of(ints, gathered) + F32(0.5) * fnum(ints[2]))
    re, im = both[:, :1024], both[:, 1024:]
    out[0] = re * fr + im * fi
    out[1] = im * fr - re * fi


def finish_kernel(x, m, out):
    rows = pmm(to_rows(receive(m, 0)), lane_moves(), True)
    other = to_lanes(pleft(row_moves(True), rows))
    out[0] = x[0] - other[:, :1024]
    out[1] = x[1] - other[:, 1024:]


def table_b_kernel(
    ints, fl, pulse, gathered, a1h, a1l, b1h, b1l, a2h, a2l, b2h, b2l, vh, vl, fmr, fmi, ffr, ffi
):
    w = 256
    lane = iota((1, w), 1)
    natural = [(lane >> 6) & 3, (lane >> 4) & 3, (lane >> 2) & 3, lane & 3]
    eye = identity(w)
    first = [rotation(ints, pulse, 0, k, w) for k in range(3)]
    second = [rotation(ints, pulse, 1, k, w) for k in range(4)]
    store_kron(a1h, a1l, [*first, eye], natural)
    store_kron(b1h, b1l, [*(flip(o) for o in first), eye], natural)
    store_kron(a2h, a2l, second, natural)
    store_kron(b2h, b2l, [flip(o) for o in second], natural)
    row = iota((16, w), 0)
    cl, l0, l1, l2, ll = (lane >> 7), (lane >> 5) & 3, (lane >> 3) & 3, (lane >> 1) & 3, lane & 1
    t0 = lane_rows(flip(second[0]), l0)
    t1 = lane_rows(flip(second[1]), l1)
    t2 = lane_rows(flip(second[2]), l2)
    low = pick((row >> 1) & 3, t2) * jnp.where((row & 1) == ll, F32(1.0), F32(0.0))
    high_bit = row >> 3
    for n in range(16):
        c, d0, top = n >> 3, (n >> 1) & 3, n & 1
        mid = jnp.where(high_bit == 0, t1[2 * top], t1[2 * top + 1])
        block = low * mid * (t0[d0] * jnp.where(cl == c, F32(1.0), F32(0.0)))
        hi, lo = split(block)
        vh[16 * n : 16 * n + 16, :] = hi
        vl[16 * n : 16 * n + 16, :] = lo
    row = iota((256, 128), 0)
    col = iota((1, 128), 1)
    rd = [fnum((row >> (6 - 2 * k)) & 3) for k in range(4)]
    cd = [fnum((col >> 5) & 3), fnum((col >> 3) & 3), fnum((col >> 1) & 3)]
    t12 = F32(0.5) * (fnum(ints[2]) + fnum(ints[3]))

    def node(k, n):
        return node_energy(fl, k, n) + fl[14 + k] * drive_weight(n)

    ai = fl[5] * (rd[0] * rd[1]) + fl[6] * (rd[1] * rd[2]) + fl[7] * (rd[2] * rd[3])
    for k in range(4):
        ai = ai + node(k, rd[k])
    aj = fl[5] * (cd[0] * cd[1]) + fl[6] * (cd[1] * cd[2])
    for k in range(3):
        aj = aj + node(k, cd[k])
    gap = None
    for k in range(3):
        part = fl[9 + k] * ((rd[k] - cd[k]) * (rd[k] - cd[k]))
        gap = part if gap is None else gap + part
    mag = jnp.exp(-t12 * gap)
    si, ci = sincos(t12 * ai)
    sj, cj = sincos(t12 * aj)
    fmr[...] = mag * (ci * cj + si * sj)
    fmi[...] = mag * (ci * sj - si * cj)
    rank = ints[4]
    i4 = fnum(jnp.full((256, 128), rank >> 3, jnp.int32))
    j3 = fnum(jnp.full((1, 128), (rank >> 1) & 3, jnp.int32))
    j4 = fnum((rank & 1) * 2 + (col & 1))
    rows = [*rd, i4]
    cols = [*cd, j3, j4]
    span = fnum(ints[3])
    time = start_of(ints, gathered) + (fnum(ints[2]) + F32(0.5) * span)
    (si, ci), (sj, cj) = factor_parts(fl, span, -1, time, rows, cols)
    mag = jnp.exp(F32(-0.5) * span * decay_of(fl, rows, cols))
    ffr[...] = mag * (ci * cj + si * sj)
    ffi[...] = mag * (ci * sj - si * cj)


def cmul(x, fr, fi, conj=False):
    re, im = x[:, :128], x[:, 128:]
    if conj:
        return jnp.concatenate([re * fr + im * fi, im * fr - re * fi], axis=1)
    return jnp.concatenate([re * fr - im * fi, re * fi + im * fr], axis=1)


def both_b_kernel(x, a1h, a1l, b1h, b1l, a2h, a2l, b2h, b2l, vh, vl, fmr, fmi, ffr, ffi, out):
    z = left(a1h[...], a1l[...], x[:, :256])
    z = cmul(z, fmr[...], fmi[...])
    z = left(a2h[...], a2l[...], z)
    z = mm(z, vh[...], vl[...])
    z = cmul(z, ffr[...], ffi[...]) - x[:, 256:]
    out[:, 256:] = z
    z = cmul(z, ffr[...], ffi[...], True)
    z = left(b2h[...], b2l[...], z)
    z = mm(z, vh[...], vl[...], True)
    z = cmul(z, fmr[...], fmi[...], True)
    out[:, :256] = left(b1h[...], b1l[...], z)


SMEM = pl.BlockSpec(memory_space=pltpu.SMEM)
VMEM = pl.BlockSpec(memory_space=pltpu.VMEM)
HBM = pl.BlockSpec(memory_space=pltpu.MemorySpace.HBM)


def with_params(kernel):
    def run(segment, tick, rank, shift, coupling, dephase, detuning, *refs):
        ints = [segment[0, 0], segment[0, 1], tick[0, 0], tick[0, 1], rank[0], rank[1]]
        sources = ((shift, 5), (coupling, 4), (dephase, 5), (detuning, 5))
        kernel(ints, [ref[n] for ref, count in sources for n in range(count)], *refs)

    return run


def call(kernel, args, scalars, outs, flops, name, far=(), scratch=()):
    specs = [SMEM if n < scalars else HBM if n in far else VMEM for n in range(len(args))]
    return pl.pallas_call(
        with_params(kernel) if scalars else kernel,
        in_specs=specs,
        out_specs=jax.tree.map(lambda _: VMEM, outs),
        out_shape=outs,
        scratch_shapes=scratch,
        name=name,
        compiler_params=pltpu.CompilerParams(vmem_limit_bytes=16 << 20),
        cost_estimate=pl.CostEstimate(flops=flops, transcendentals=0, bytes_accessed=1 << 20),
    )(*args)


def sds(*shape, dtype=F32):
    return jax.ShapeDtypeStruct(shape, dtype)


def local(linkage, pulse, segments, ticks, detuning, level_shift, coupling, dephase):
    current = linkage[:, 0]
    phases = lax.axis_size("phase")
    rank = jnp.stack([lax.axis_index("row"), lax.axis_index("phase")]).astype(jnp.int32)
    params = (segments, ticks, rank, level_shift, coupling, dephase, detuning)
    angles = jnp.transpose(pulse, (1, 2, 0))
    gathered = lax.all_to_all(
        jnp.broadcast_to(ticks, (phases, STEPS)), "phase", split_axis=0, concat_axis=0, tiled=True
    )
    def turn(x):
        return lax.all_to_all(
            x.reshape(32, 8, 512), "row", split_axis=0, concat_axis=0, tiled=True
        )

    following = lax.ppermute(current, "phase", [((i + 1) % phases, i) for i in range(phases)])
    following = call(raw_kernel, (following,), 0, sds(32, 8, 256), 1 << 26, "raw")
    square = sds(256, 256, dtype=BF16)
    *tables_a, weighed = call(
        table_a_kernel,
        (
            *params,
            angles,
            pltpu.with_memory_space_constraint(current, pltpu.MemorySpace.HBM),
        ),
        8,
        (
            *([square] * 6),
            sds(32, 128),
            sds(32, 128),
            sds(16, 256),
            sds(2, 32, 1024),
        ),
        1 << 28,
        "table_a",
        far=(8,),
        scratch=(pltpu.VMEM((2, 32, 1024), F32), pltpu.SemaphoreType.DMA),
    )
    sent = call(
        forward_a_kernel,
        (*params, gathered, weighed, following, *tables_a),
        7,
        sds(32, 8, 512),
        1 << 28,
        "forward_a",
    )
    turned = turn(sent)
    tables_b = call(
        table_b_kernel,
        (*params, angles, gathered),
        8,
        (*([square] * 10), *([sds(256, 128)] * 4)),
        1 << 28,
        "table_b",
    )
    back = call(
        both_b_kernel,
        (turned.reshape(256, 512), *tables_b),
        0,
        sds(256, 512),
        1 << 28,
        "both_b",
    )
    returned = turn(back)
    earlier = lax.ppermute(
        returned[:, :, 256:], "phase", [(i, (i + 1) % phases) for i in range(phases)]
    )
    costate = call(
        adjoint_a_kernel,
        (*params, angles, gathered, returned, *tables_a[:4], *tables_a[6:]),
        8,
        sds(2, 32, 1024),
        1 << 28,
        "adjoint_a",
        scratch=(pltpu.VMEM((256, 256), BF16), pltpu.VMEM((256, 256), BF16)),
    )
    result = call(finish_kernel, (costate, earlier), 0, sds(2, 32, 1024), 1 << 26, "finish")
    return result[:, None]


def solution(mesh):
    return jax.shard_map(
        local,
        mesh=mesh,
        in_specs=(
            P(None, "phase", "row", None),
            P(),
            P("phase", None),
            P("phase", None),
            P(),
            P(),
            P(),
            P(),
        ),
        out_specs=P(None, "phase", "row", None),
        check_vma=False,
    )
```

```python
import math

import jax
import jax.numpy as jnp
from jax import lax
from jax.experimental import pallas as pl
from jax.experimental.pallas import tpu as pltpu
from jax.sharding import PartitionSpec as P

TRANSMONS = 5
LEVELS = 4
STEPS = 2


F32 = jnp.float32
BF16 = jnp.bfloat16


def iota(shape, dim):
    return lax.broadcasted_iota(jnp.int32, shape, dim)


def sincos(x):
    q = jnp.floor(x * F32(2.0 / math.pi) + F32(0.5))
    r = x - q * F32(1.5703125)
    r = r - q * F32(4.837512969970703125e-4)
    r = r - q * F32(7.549789948768648e-8)
    z = r * r
    s = r + r * z * (F32(-1 / 6) + z * (F32(1 / 120) + z * (F32(-1 / 5040) + z * F32(1 / 362880))))
    c = F32(1.0) + z * (
        F32(-0.5) + z * (F32(1 / 24) + z * (F32(-1 / 720) + z * F32(1 / 40320)))
    )
    k = q.astype(jnp.int32)
    odd = (k & 1) == 1
    sin = jnp.where(odd, c, s)
    cos = jnp.where(odd, s, c)
    sin = jnp.where((k & 2) == 2, -sin, sin)
    cos = jnp.where(((k + 1) & 2) == 2, -cos, cos)
    return sin, cos


def split(x):
    hi = x.astype(BF16)
    return hi, (x - hi.astype(F32)).astype(BF16)


def dot(a, b, transposed=False):
    dims = (((1,), (1 if transposed else 0,)), ((), ()))
    return lax.dot_general(a, b, dims, preferred_element_type=F32)


def mm(x, hi, lo, transposed=False):
    a, b = split(x)
    tables = jnp.concatenate([hi, lo, hi], axis=1 if transposed else 0)
    return dot(jnp.concatenate([a, a, b], axis=1), tables, transposed)


def left(hi, lo, x):
    a, b = split(x)
    return dot(jnp.concatenate([hi, hi, lo], axis=1), jnp.concatenate([a, b, a], axis=0))


def pmm(x, w, transposed=False):
    a, b = split(x)
    return dot(a, w, transposed) + dot(b, w, transposed)


def pleft(w, x):
    return dot(jnp.concatenate([w, w], axis=1), jnp.concatenate(split(x), axis=0))


def rotation(ints, pulse, step, k, width):
    sc = [sincos(jnp.full((1, width), pulse[k, m, ints[step]], F32)) for m in range(3)]
    (s0, c0), (s1, c1), (s2, c2) = sc
    zero = jnp.zeros((1, width), F32)
    return [
        [c0, -s0 * c1, s0 * s1 * c2, -s0 * s1 * s2],
        [s0, c0 * c1, -c0 * s1 * c2, c0 * s1 * s2],
        [zero, s1, c1 * c2, -c1 * s2],
        [zero, zero, s2, c2],
    ]


def identity(width):
    one, zero = jnp.ones((1, width), F32), jnp.zeros((1, width), F32)
    return [[one if a == b else zero for b in range(4)] for a in range(4)]


def flip(o):
    return [[o[b][a] for b in range(4)] for a in range(4)]


def pick(digit, choices):
    out = choices[3]
    for v in (2, 1, 0):
        out = jnp.where(digit == v, choices[v], out)
    return out


def lane_rows(o, lane_digit):
    return [pick(lane_digit, o[x]) for x in range(4)]


def kron_blocks(mats, lane_digits):
    width = lane_digits[0].shape[1]
    t = [lane_rows(o, d) for o, d in zip(mats, lane_digits)]
    row = iota((16, width), 0)
    low = pick(row >> 2, t[2]) * pick(row & 3, t[3])
    return [low * (t[0][a] * t[1][b]) for a in range(4) for b in range(4)]


def store_kron(hi_ref, lo_ref, mats, lane_digits):
    for n, block in enumerate(kron_blocks(mats, lane_digits)):
        hi, lo = split(block)
        hi_ref[16 * n : 16 * n + 16, :] = hi
        lo_ref[16 * n : 16 * n + 16, :] = lo


def fnum(x):
    return x.astype(F32)


def node_energy(fl, k, n):
    return fl[k] * (n * (n - F32(1.0)) * F32(0.5))


def drive_weight(n):
    return n * (n + F32(1.0)) * F32(0.5)


def moved_lanes(lane):
    return [
        (lane >> 3) & 3,
        (lane >> 1) & 3,
        (lane >> 6) & 3,
        ((lane >> 5) & 1) * 2 + (lane & 1),
    ]


def lane_moves():
    j1, j2, j3, j4 = moved_lanes(iota((1, 256), 1))
    lanes = iota((256, 256), 0) == j1 * 64 + j2 * 16 + j3 * 4 + j4
    return jnp.where(lanes, F32(1.0), F32(0.0)).astype(BF16)


def moved_row(m):
    return (m & ~31) + ((m >> 2) & 1) * 16 + (m & 3) * 4 + ((m >> 3) & 3)


def row_moves(back):
    if back:
        rows = iota((256, 256), 0) == moved_row(iota((1, 256), 1))
    else:
        rows = moved_row(iota((256, 1), 0)) == iota((256, 256), 1)
    return jnp.where(rows, F32(1.0), F32(0.0)).astype(BF16)


def store_rows_a(hi_ref, lo_ref, o0, o3, o4):
    lane = iota((1, 256), 1)
    row = iota((16, 256), 0)
    t0, t3, t4 = (
        lane_rows(o, d) for o, d in ((o0, (lane >> 6) & 3), (o3, (lane >> 2) & 3), (o4, lane & 3))
    )
    same = ((row >> 2) & 1) == ((lane >> 4) & 1)
    low = pick(row & 3, t3) * jnp.where(same, F32(1.0), F32(0.0))
    mid = [low * jnp.where((row >> 3) == 0, t4[2 * h], t4[2 * h + 1]) for h in range(2)]
    for n in range(16):
        kept = jnp.where(((lane >> 5) & 1) == ((n >> 1) & 1), F32(1.0), F32(0.0))
        hi, lo = split(mid[n & 1] * (t0[n >> 2] * kept))
        hi_ref[16 * n : 16 * n + 16, :] = hi
        lo_ref[16 * n : 16 * n + 16, :] = lo


def table_a_kernel(
    ints, fl, pulse, source, w1h, w1l, w2h, w2l, k1h, k1l, far, fai, o4, gx, x, sem
):
    fetch = pltpu.make_async_copy(source, x, sem)
    fetch.start()
    w = 256
    lane = iota((1, w), 1)
    natural = [(lane >> 6) & 3, (lane >> 4) & 3, (lane >> 2) & 3, lane & 3]
    moved = moved_lanes(lane)
    eye = identity(w)
    first = [rotation(ints, pulse, 0, k, w) for k in range(TRANSMONS)]
    second = {k: rotation(ints, pulse, 1, k, w) for k in (3, 4)}
    store_kron(w1h, w1l, [flip(first[k]) for k in (1, 2, 3, 4)], natural)
    store_kron(w2h, w2l, [eye, eye, flip(second[3]), flip(second[4])], moved)
    store_rows_a(k1h, k1l, first[0], first[3], first[4])
    for a in range(4):
        for b in range(4):
            o4[4 * a + b : 4 * a + b + 1, :] = second[4][a][b]
    t12 = F32(0.5) * (fnum(ints[2]) + fnum(ints[3]))
    row = iota((32, 128), 0)
    col = iota((1, 128), 1)
    i3, i4 = fnum(row & 3), fnum(row >> 3)
    j2, j3, j4 = fnum((col >> 4) & 3), fnum((col >> 2) & 3), fnum(col & 3)

    def node(k, n):
        return node_energy(fl, k, n) + fl[14 + k] * drive_weight(n)

    ai = t12 * (fl[8] * (i3 * i4) + node(4, i4))
    aj = t12 * (fl[7] * (j2 * j3) + fl[8] * (j3 * j4) + node(3, j3) + node(4, j4))
    mag = jnp.exp(
        -t12 * (fl[12] * ((i3 - j3) * (i3 - j3)) + fl[13] * ((i4 - j4) * (i4 - j4)))
    )
    si, ci = sincos(ai)
    sj, cj = sincos(aj)
    far[...] = mag * (ci * cj + si * sj)
    fai[...] = mag * (ci * sj - si * cj)
    fr, fi = first_factor(ints, fl, F32(0.5) * fnum(ints[2]))
    fetch.wait()
    re, im = x[0], x[1]
    gx[0] = re * fr - im * fi
    gx[1] = re * fi + im * fr


def first_factor(ints, fl, time):
    span = fnum(ints[2])
    rd, cd = digits_a(ints)
    (si, ci), (sj, cj) = factor_parts(fl, span, 1, time, rd, cd)
    wide = [jnp.concatenate([d] * 8, axis=1) for d in rd]
    mag = jnp.exp(F32(-0.5) * span * decay_of(fl, wide, cd))
    si, ci = jnp.concatenate([si] * 8, axis=1), jnp.concatenate([ci] * 8, axis=1)
    return mag * (ci * cj + si * sj), mag * (ci * sj - si * cj)


def digits_a(ints):
    row = ints[4] * 32 + iota((32, 128), 0)
    col = iota((1, 1024), 1)
    rd = [fnum((row >> (8 - 2 * k)) & 3) for k in range(TRANSMONS)]
    cd = [fnum((col >> (8 - 2 * k)) & 3) for k in range(TRANSMONS)]
    return rd, cd


def start_of(ints, gathered):
    rows = iota((8, 2), 0)
    kept = jnp.where(rows < ints[5], gathered[...], 0).astype(F32)
    return jnp.sum(jnp.sum(kept, axis=1, keepdims=True), axis=0, keepdims=True)


def drive_phase(fl, k, time):
    phi = time * fl[14 + k]
    turns = jnp.floor(phi * F32(0.5 / math.pi) + F32(0.5))
    return phi - turns * F32(6.28125) - turns * F32(2 * math.pi - 6.28125)


def energy_of(fl, digits):
    total = node_energy(fl, 0, digits[0])
    for k in range(1, TRANSMONS):
        total = total + node_energy(fl, k, digits[k])
    for k in range(TRANSMONS - 1):
        total = total + fl[5 + k] * (digits[k] * digits[k + 1])
    return total


def factor_parts(fl, span, sign, time, row_digits, col_digits):
    phis = [drive_phase(fl, k, time) for k in range(TRANSMONS)]

    def angle(digits):
        total = (F32(0.5) * span) * energy_of(fl, digits)
        drive = phis[0] * drive_weight(digits[0])
        for k in range(1, TRANSMONS):
            drive = drive + phis[k] * drive_weight(digits[k])
        return total + drive if sign > 0 else total - drive

    return sincos(angle(row_digits)), sincos(angle(col_digits))


def decay_of(fl, row_digits, col_digits):
    total = None
    for k in range(TRANSMONS):
        gap = row_digits[k] - col_digits[k]
        part = fl[9 + k] * (gap * gap)
        total = part if total is None else total + part
    return total


def start_factor(ints, fl, gathered):
    time = start_of(ints, gathered)
    rd, cd = digits_a(ints)
    phis = [drive_phase(fl, k, time) for k in range(TRANSMONS)]

    def angle(digits):
        total = phis[0] * drive_weight(digits[0])
        for k in range(1, TRANSMONS):
            total = total + phis[k] * drive_weight(digits[k])
        return total

    si, ci = sincos(angle(rd))
    sj, cj = sincos(angle(cd))
    si, ci = jnp.concatenate([si] * 8, axis=1), jnp.concatenate([ci] * 8, axis=1)
    return ci * cj + si * sj, ci * sj - si * cj


def to_rows(blocks):
    return jnp.concatenate(
        [
            blocks[:, c * 1024 + a * 256 : c * 1024 + a * 256 + 256]
            for a in range(4)
            for c in range(2)
        ],
        axis=0,
    )


def to_lanes(rows):
    return jnp.concatenate(
        [rows[(2 * a + c) * 32 : (2 * a + c) * 32 + 32, :] for c in range(2) for a in range(4)],
        axis=1,
    )


def mix_i4(o4, rows, transposed):
    parts = [
        jnp.concatenate([rows[32 * n + 8 * b : 32 * n + 8 * b + 8, :] for n in range(8)], axis=0)
        for b in range(4)
    ]
    out = []
    for a in range(4):
        total = None
        for b in range(4):
            n = 4 * b + a if transposed else 4 * a + b
            part = parts[b] * o4[n : n + 1, :]
            total = part if total is None else total + part
        out.append(total)
    return jnp.concatenate(
        [out[a][8 * n : 8 * n + 8, :] for n in range(8) for a in range(4)], axis=0
    )


def chunk_of_lane(shape):
    return (iota(shape, 1) >> 5) & 3


def send(out, offset, x):
    for c in range(2):
        for half in range(2):
            tiles = [
                x[:, c * 1024 + a * 256 + half * 128 : c * 1024 + a * 256 + half * 128 + 128]
                for a in range(4)
            ]
            chunk = chunk_of_lane((32, 128))
            for q in range(4):
                moved = [
                    tiles[a] if a == q else pltpu.roll(tiles[a], ((a - q) * 32) % 128, 1)
                    for a in range(4)
                ]
                merged = pick(chunk, moved)
                for i4 in range(4):
                    out[i4 * 8 + half * 4 + q, :, offset + c * 128 : offset + c * 128 + 128] = (
                        merged[i4 * 8 : i4 * 8 + 8, :]
                    )


def receive(ref, offset):
    chunk = chunk_of_lane((32, 128))
    pieces = {}
    for c in range(2):
        for half in range(2):
            merged = [
                jnp.concatenate(
                    [
                        ref[i4 * 8 + half * 4 + q, :, offset + c * 128 : offset + c * 128 + 128]
                        for i4 in range(4)
                    ],
                    axis=0,
                )
                for q in range(4)
            ]
            for a in range(4):
                moved = [
                    merged[q] if a == q else pltpu.roll(merged[q], ((q - a) * 32) % 128, 1)
                    for q in range(4)
                ]
                pieces[c, a, half] = pick(chunk, moved)
    return jnp.concatenate(
        [pieces[c, a, half] for c in range(2) for a in range(4) for half in range(2)], axis=1
    )


def apply_pointwise_a(rows, far, fai, conj):
    fr = jnp.concatenate([far, far], axis=1)
    fi = jnp.concatenate([fai, fai], axis=1)
    if conj:
        fi = -fi
    out = []
    for a in range(4):
        re, im = rows[64 * a : 64 * a + 32, :], rows[64 * a + 32 : 64 * a + 64, :]
        out += [re * fr - im * fi, re * fi + im * fr]
    return jnp.concatenate(out, axis=0)


def raw_kernel(x, out):
    rows = to_rows(jnp.concatenate([x[0], x[1]], axis=1))
    send(out, 0, to_lanes(pmm(pleft(row_moves(False), rows), lane_moves())))


def forward_a_kernel(
    ints, fl, gathered, gx, other, w1h, w1l, w2h, w2l, k1h, k1l, far, fai, o4, out
):
    out[:, :, 256:] = other[...]
    fr, fi = start_factor(ints, fl, gathered)
    re, im = gx[0], gx[1]
    rows = to_rows(jnp.concatenate([re * fr - im * fi, re * fi + im * fr], axis=1))
    rows = mm(left(k1h[...], k1l[...], rows), w1h[...], w1l[...])
    rows = apply_pointwise_a(rows, far[...], fai[...], False)
    send(out, 0, to_lanes(mm(mix_i4(o4, rows, False), w2h[...], w2l[...])))


def adjoint_a_kernel(
    ints, fl, pulse, gathered, y, w1h, w1l, w2h, w2l, far, fai, o4, out, t1h, t1l
):
    rows = mm(to_rows(receive(y, 0)), w2h[...], w2l[...], True)
    rows = apply_pointwise_a(mix_i4(o4, rows, True), far[...], fai[...], True)
    rows = mm(rows, w1h[...], w1l[...], True)
    lane = iota((1, 256), 1)
    sent = [
        (lane >> 6) & 3,
        ((lane >> 5) & 1) * 2 + ((lane >> 2) & 1),
        lane & 3,
        (lane >> 3) & 3,
    ]
    first = [flip(rotation(ints, pulse, 0, k, 256)) for k in (0, 3, 4)]
    store_kron(t1h, t1l, [first[0], identity(256), first[1], first[2]], sent)
    both = to_lanes(left(t1h[...], t1l[...], rows))
    fr, fi = first_factor(ints, fl, start_of(ints, gathered) + F32(0.5) * fnum(ints[2]))
    re, im = both[:, :1024], both[:, 1024:]
    out[0] = re * fr + im * fi
    out[1] = im * fr - re * fi


def finish_kernel(x, m, out):
    rows = pmm(to_rows(receive(m, 0)), lane_moves(), True)
    other = to_lanes(pleft(row_moves(True), rows))
    out[0] = x[0] - other[:, :1024]
    out[1] = x[1] - other[:, 1024:]


def table_b_kernel(
    ints, fl, pulse, gathered, a1h, a1l, b1h, b1l, a2h, a2l, b2h, b2l, vh, vl, fmr, fmi, ffr, ffi
):
    w = 256
    lane = iota((1, w), 1)
    natural = [(lane >> 6) & 3, (lane >> 4) & 3, (lane >> 2) & 3, lane & 3]
    eye = identity(w)
    first = [rotation(ints, pulse, 0, k, w) for k in range(3)]
    second = [rotation(ints, pulse, 1, k, w) for k in range(4)]
    store_kron(a1h, a1l, [*first, eye], natural)
    store_kron(b1h, b1l, [*(flip(o) for o in first), eye], natural)
    store_kron(a2h, a2l, second, natural)
    store_kron(b2h, b2l, [flip(o) for o in second], natural)
    row = iota((16, w), 0)
    cl, l0, l1, l2, ll = (lane >> 7), (lane >> 5) & 3, (lane >> 3) & 3, (lane >> 1) & 3, lane & 1
    t0 = lane_rows(flip(second[0]), l0)
    t1 = lane_rows(flip(second[1]), l1)
    t2 = lane_rows(flip(second[2]), l2)
    low = pick((row >> 1) & 3, t2) * jnp.where((row & 1) == ll, F32(1.0), F32(0.0))
    high_bit = row >> 3
    for n in range(16):
        c, d0, top = n >> 3, (n >> 1) & 3, n & 1
        mid = jnp.where(high_bit == 0, t1[2 * top], t1[2 * top + 1])
        block = low * mid * (t0[d0] * jnp.where(cl == c, F32(1.0), F32(0.0)))
        hi, lo = split(block)
        vh[16 * n : 16 * n + 16, :] = hi
        vl[16 * n : 16 * n + 16, :] = lo
    row = iota((256, 128), 0)
    col = iota((1, 128), 1)
    rd = [fnum((row >> (6 - 2 * k)) & 3) for k in range(4)]
    cd = [fnum((col >> 5) & 3), fnum((col >> 3) & 3), fnum((col >> 1) & 3)]
    t12 = F32(0.5) * (fnum(ints[2]) + fnum(ints[3]))

    def node(k, n):
        return node_energy(fl, k, n) + fl[14 + k] * drive_weight(n)

    ai = fl[5] * (rd[0] * rd[1]) + fl[6] * (rd[1] * rd[2]) + fl[7] * (rd[2] * rd[3])
    for k in range(4):
        ai = ai + node(k, rd[k])
    aj = fl[5] * (cd[0] * cd[1]) + fl[6] * (cd[1] * cd[2])
    for k in range(3):
        aj = aj + node(k, cd[k])
    gap = None
    for k in range(3):
        part = fl[9 + k] * ((rd[k] - cd[k]) * (rd[k] - cd[k]))
        gap = part if gap is None else gap + part
    mag = jnp.exp(-t12 * gap)
    si, ci = sincos(t12 * ai)
    sj, cj = sincos(t12 * aj)
    fmr[...] = mag * (ci * cj + si * sj)
    fmi[...] = mag * (ci * sj - si * cj)
    rank = ints[4]
    i4 = fnum(jnp.full((256, 128), rank >> 3, jnp.int32))
    j3 = fnum(jnp.full((1, 128), (rank >> 1) & 3, jnp.int32))
    j4 = fnum((rank & 1) * 2 + (col & 1))
    rows = [*rd, i4]
    cols = [*cd, j3, j4]
    span = fnum(ints[3])
    time = start_of(ints, gathered) + (fnum(ints[2]) + F32(0.5) * span)
    (si, ci), (sj, cj) = factor_parts(fl, span, -1, time, rows, cols)
    mag = jnp.exp(F32(-0.5) * span * decay_of(fl, rows, cols))
    ffr[...] = mag * (ci * cj + si * sj)
    ffi[...] = mag * (ci * sj - si * cj)


def cmul(x, fr, fi, conj=False):
    re, im = x[:, :128], x[:, 128:]
    if conj:
        return jnp.concatenate([re * fr + im * fi, im * fr - re * fi], axis=1)
    return jnp.concatenate([re * fr - im * fi, re * fi + im * fr], axis=1)


def both_b_kernel(x, a1h, a1l, b1h, b1l, a2h, a2l, b2h, b2l, vh, vl, fmr, fmi, ffr, ffi, out):
    z = left(a1h[...], a1l[...], x[:, :256])
    z = cmul(z, fmr[...], fmi[...])
    z = left(a2h[...], a2l[...], z)
    z = mm(z, vh[...], vl[...])
    z = cmul(z, ffr[...], ffi[...]) - x[:, 256:]
    out[:, 256:] = z
    z = cmul(z, ffr[...], ffi[...], True)
    z = left(b2h[...], b2l[...], z)
    z = mm(z, vh[...], vl[...], True)
    z = cmul(z, fmr[...], fmi[...], True)
    out[:, :256] = left(b1h[...], b1l[...], z)


SMEM = pl.BlockSpec(memory_space=pltpu.SMEM)
VMEM = pl.BlockSpec(memory_space=pltpu.VMEM)
HBM = pl.BlockSpec(memory_space=pltpu.MemorySpace.HBM)


def with_params(kernel):
    def run(segment, tick, rank, shift, coupling, dephase, detuning, *refs):
        ints = [segment[0, 0], segment[0, 1], tick[0, 0], tick[0, 1], rank[0], rank[1]]
        sources = ((shift, 5), (coupling, 4), (dephase, 5), (detuning, 5))
        kernel(ints, [ref[n] for ref, count in sources for n in range(count)], *refs)

    return run


def call(kernel, args, scalars, outs, flops, name, far=(), scratch=()):
    specs = [SMEM if n < scalars else HBM if n in far else VMEM for n in range(len(args))]
    return pl.pallas_call(
        with_params(kernel) if scalars else kernel,
        in_specs=specs,
        out_specs=jax.tree.map(lambda _: VMEM, outs),
        out_shape=outs,
        scratch_shapes=scratch,
        name=name,
        compiler_params=pltpu.CompilerParams(vmem_limit_bytes=16 << 20),
        cost_estimate=pl.CostEstimate(flops=flops, transcendentals=0, bytes_accessed=1 << 20),
    )(*args)


def sds(*shape, dtype=F32):
    return jax.ShapeDtypeStruct(shape, dtype)


def local(linkage, pulse, segments, ticks, detuning, level_shift, coupling, dephase):
    current = linkage[:, 0]
    phases = lax.axis_size("phase")
    rank = jnp.stack([lax.axis_index("row"), lax.axis_index("phase")]).astype(jnp.int32)
    params = (segments, ticks, rank, level_shift, coupling, dephase, detuning)
    angles = jnp.transpose(pulse, (1, 2, 0))
    gathered = lax.all_to_all(
        jnp.broadcast_to(ticks, (phases, STEPS)), "phase", split_axis=0, concat_axis=0, tiled=True
    )
    def turn(x):
        return lax.all_to_all(
            x.reshape(32, 8, 512), "row", split_axis=0, concat_axis=0, tiled=True
        )

    following = lax.ppermute(current, "phase", [((i + 1) % phases, i) for i in range(phases)])
    following = call(raw_kernel, (following,), 0, sds(32, 8, 256), 1 << 26, "raw")
    square = sds(256, 256, dtype=BF16)
    *tables_a, weighed = call(
        table_a_kernel,
        (
            *params,
            angles,
            pltpu.with_memory_space_constraint(current, pltpu.MemorySpace.HBM),
        ),
        8,
        (
            *([square] * 6),
            sds(32, 128),
            sds(32, 128),
            sds(16, 256),
            sds(2, 32, 1024),
        ),
        1 << 28,
        "table_a",
        far=(8,),
        scratch=(pltpu.VMEM((2, 32, 1024), F32), pltpu.SemaphoreType.DMA),
    )
    sent = call(
        forward_a_kernel,
        (*params, gathered, weighed, following, *tables_a),
        7,
        sds(32, 8, 512),
        1 << 28,
        "forward_a",
    )
    turned = turn(sent)
    tables_b = call(
        table_b_kernel,
        (*params, angles, gathered),
        8,
        (*([square] * 10), *([sds(256, 128)] * 4)),
        1 << 28,
        "table_b",
    )
    back = call(
        both_b_kernel,
        (turned.reshape(256, 512), *tables_b),
        0,
        sds(256, 512),
        1 << 28,
        "both_b",
    )
    returned = turn(back)
    earlier = lax.ppermute(
        returned[:, :, 256:], "phase", [(i, (i + 1) % phases) for i in range(phases)]
    )
    costate = call(
        adjoint_a_kernel,
        (*params, angles, gathered, returned, *tables_a[:4], *tables_a[6:]),
        8,
        sds(2, 32, 1024),
        1 << 28,
        "adjoint_a",
        scratch=(pltpu.VMEM((256, 256), BF16), pltpu.VMEM((256, 256), BF16)),
    )
    result = call(finish_kernel, (costate, earlier), 0, sds(2, 32, 1024), 1 << 26, "finish")
    return result[:, None]


def solution(mesh):
    return jax.shard_map(
        local,
        mesh=mesh,
        in_specs=(
            P(None, "phase", "row", None),
            P(),
            P("phase", None),
            P("phase", None),
            P(),
            P(),
            P(),
            P(),
        ),
        out_specs=P(None, "phase", "row", None),
        check_vma=False,
    )
```

```python
import math

import jax
import jax.numpy as jnp
from jax import lax
from jax.experimental import pallas as pl
from jax.experimental.pallas import tpu as pltpu
from jax.sharding import PartitionSpec as P

TRANSMONS = 5
LEVELS = 4
STEPS = 2


F32 = jnp.float32
BF16 = jnp.bfloat16


def iota(shape, dim):
    return lax.broadcasted_iota(jnp.int32, shape, dim)


def sincos(x):
    q = jnp.floor(x * F32(2.0 / math.pi) + F32(0.5))
    r = x - q * F32(1.5703125)
    r = r - q * F32(4.837512969970703125e-4)
    r = r - q * F32(7.549789948768648e-8)
    z = r * r
    s = r + r * z * (F32(-1 / 6) + z * (F32(1 / 120) + z * (F32(-1 / 5040) + z * F32(1 / 362880))))
    c = F32(1.0) + z * (
        F32(-0.5) + z * (F32(1 / 24) + z * (F32(-1 / 720) + z * F32(1 / 40320)))
    )
    k = q.astype(jnp.int32)
    odd = (k & 1) == 1
    sin = jnp.where(odd, c, s)
    cos = jnp.where(odd, s, c)
    sin = jnp.where((k & 2) == 2, -sin, sin)
    cos = jnp.where(((k + 1) & 2) == 2, -cos, cos)
    return sin, cos


def split(x):
    hi = x.astype(BF16)
    return hi, (x - hi.astype(F32)).astype(BF16)


def dot(a, b, transposed=False):
    dims = (((1,), (1 if transposed else 0,)), ((), ()))
    return lax.dot_general(a, b, dims, preferred_element_type=F32)


def mm(x, hi, lo, transposed=False):
    a, b = split(x)
    tables = jnp.concatenate([hi, lo, hi], axis=1 if transposed else 0)
    return dot(jnp.concatenate([a, a, b], axis=1), tables, transposed)


def left(hi, lo, x):
    a, b = split(x)
    return dot(jnp.concatenate([hi, hi, lo], axis=1), jnp.concatenate([a, b, a], axis=0))


def pmm(x, w, transposed=False):
    a, b = split(x)
    return dot(a, w, transposed) + dot(b, w, transposed)


def pleft(w, x):
    return dot(jnp.concatenate([w, w], axis=1), jnp.concatenate(split(x), axis=0))


def rotations(ints, pulse, which, width):
    count = -(-3 * len(which) // 8) * 8
    row = iota((count, 128), 0)
    theta = jnp.zeros((count, 128), F32)
    for n, (step, k) in enumerate(which):
        for m in range(3):
            theta = jnp.where(row == 3 * n + m, pulse[k, m, ints[step]], theta)
    sines, cosines = sincos(theta)
    zero = jnp.zeros((1, width), F32)

    def splat(table, n):
        return jnp.concatenate([table[n : n + 1, :]] * (width // 128), axis=1)

    out = []
    for n in range(len(which)):
        s0, s1, s2 = (splat(sines, 3 * n + m) for m in range(3))
        c0, c1, c2 = (splat(cosines, 3 * n + m) for m in range(3))
        out.append(
            [
                [c0, -s0 * c1, s0 * s1 * c2, -s0 * s1 * s2],
                [s0, c0 * c1, -c0 * s1 * c2, c0 * s1 * s2],
                [zero, s1, c1 * c2, -c1 * s2],
                [zero, zero, s2, c2],
            ]
        )
    return out


def identity(width):
    one, zero = jnp.ones((1, width), F32), jnp.zeros((1, width), F32)
    return [[one if a == b else zero for b in range(4)] for a in range(4)]


def flip(o):
    return [[o[b][a] for b in range(4)] for a in range(4)]


def pick(digit, choices):
    out = choices[3]
    for v in (2, 1, 0):
        out = jnp.where(digit == v, choices[v], out)
    return out


def lane_rows(o, lane_digit):
    return [pick(lane_digit, o[x]) for x in range(4)]


def kron_blocks(mats, lane_digits):
    width = lane_digits[0].shape[1]
    t = [lane_rows(o, d) for o, d in zip(mats, lane_digits)]
    row = iota((16, width), 0)
    low = pick(row >> 2, t[2]) * pick(row & 3, t[3])
    return [low * (t[0][a] * t[1][b]) for a in range(4) for b in range(4)]


def store_kron(hi_ref, lo_ref, mats, lane_digits):
    for n, block in enumerate(kron_blocks(mats, lane_digits)):
        hi, lo = split(block)
        hi_ref[16 * n : 16 * n + 16, :] = hi
        lo_ref[16 * n : 16 * n + 16, :] = lo


def fnum(x):
    return x.astype(F32)


def node_energy(fl, k, n):
    return fl[k] * (n * (n - F32(1.0)) * F32(0.5))


def drive_weight(n):
    return n * (n + F32(1.0)) * F32(0.5)


def moved_lanes(lane):
    return [
        (lane >> 3) & 3,
        (lane >> 1) & 3,
        (lane >> 6) & 3,
        ((lane >> 5) & 1) * 2 + (lane & 1),
    ]


def lane_moves():
    j1, j2, j3, j4 = moved_lanes(iota((1, 256), 1))
    lanes = iota((256, 256), 0) == j1 * 64 + j2 * 16 + j3 * 4 + j4
    return jnp.where(lanes, F32(1.0), F32(0.0)).astype(BF16)


def moved_row(m):
    return (m & ~31) + ((m >> 2) & 1) * 16 + (m & 3) * 4 + ((m >> 3) & 3)


def row_moves(back):
    if back:
        rows = iota((256, 256), 0) == moved_row(iota((1, 256), 1))
    else:
        rows = moved_row(iota((256, 1), 0)) == iota((256, 256), 1)
    return jnp.where(rows, F32(1.0), F32(0.0)).astype(BF16)


def store_rows_a(hi_ref, lo_ref, o0, o3, o4):
    lane = iota((1, 256), 1)
    row = iota((16, 256), 0)
    t0, t3, t4 = (
        lane_rows(o, d) for o, d in ((o0, (lane >> 6) & 3), (o3, (lane >> 2) & 3), (o4, lane & 3))
    )
    same = ((row >> 2) & 1) == ((lane >> 4) & 1)
    low = pick(row & 3, t3) * jnp.where(same, F32(1.0), F32(0.0))
    mid = [low * jnp.where((row >> 3) == 0, t4[2 * h], t4[2 * h + 1]) for h in range(2)]
    for n in range(16):
        kept = jnp.where(((lane >> 5) & 1) == ((n >> 1) & 1), F32(1.0), F32(0.0))
        hi, lo = split(mid[n & 1] * (t0[n >> 2] * kept))
        hi_ref[16 * n : 16 * n + 16, :] = hi
        lo_ref[16 * n : 16 * n + 16, :] = lo


def table_a_kernel(
    ints, fl, pulse, source, w1h, w1l, w2h, w2l, k1h, k1l, far, fai, o4, gx, x, sem
):
    fetch = pltpu.make_async_copy(source, x, sem)
    fetch.start()
    w = 256
    lane = iota((1, w), 1)
    natural = [(lane >> 6) & 3, (lane >> 4) & 3, (lane >> 2) & 3, lane & 3]
    moved = moved_lanes(lane)
    eye = identity(w)
    which = [(0, k) for k in range(TRANSMONS)] + [(1, 3), (1, 4)]
    *first, third, fourth = rotations(ints, pulse, which, w)
    second = {3: third, 4: fourth}
    store_kron(w1h, w1l, [flip(first[k]) for k in (1, 2, 3, 4)], natural)
    store_kron(w2h, w2l, [eye, eye, flip(second[3]), flip(second[4])], moved)
    store_rows_a(k1h, k1l, first[0], first[3], first[4])
    for a in range(4):
        for b in range(4):
            o4[4 * a + b : 4 * a + b + 1, :] = second[4][a][b]
    t12 = F32(0.5) * (fnum(ints[2]) + fnum(ints[3]))
    row = iota((32, 128), 0)
    col = iota((1, 128), 1)
    i3, i4 = fnum(row & 3), fnum(row >> 3)
    j2, j3, j4 = fnum((col >> 4) & 3), fnum((col >> 2) & 3), fnum(col & 3)

    def node(k, n):
        return node_energy(fl, k, n) + fl[14 + k] * drive_weight(n)

    ai = t12 * (fl[8] * (i3 * i4) + node(4, i4))
    aj = t12 * (fl[7] * (j2 * j3) + fl[8] * (j3 * j4) + node(3, j3) + node(4, j4))
    mag = jnp.exp(
        -t12 * (fl[12] * ((i3 - j3) * (i3 - j3)) + fl[13] * ((i4 - j4) * (i4 - j4)))
    )
    si, ci = sincos(ai)
    sj, cj = sincos(aj)
    far[...] = mag * (ci * cj + si * sj)
    fai[...] = mag * (ci * sj - si * cj)
    fr, fi = first_factor(ints, fl, F32(0.5) * fnum(ints[2]))
    fetch.wait()
    re, im = x[0], x[1]
    gx[0] = re * fr - im * fi
    gx[1] = re * fi + im * fr


def first_factor(ints, fl, time):
    span = fnum(ints[2])
    rd, cd = digits_a(ints)
    (si, ci), (sj, cj) = factor_parts(fl, span, 1, time, rd, cd)
    wide = [jnp.concatenate([d] * 8, axis=1) for d in rd]
    mag = jnp.exp(F32(-0.5) * span * decay_of(fl, wide, cd))
    si, ci = jnp.concatenate([si] * 8, axis=1), jnp.concatenate([ci] * 8, axis=1)
    return mag * (ci * cj + si * sj), mag * (ci * sj - si * cj)


def digits_a(ints):
    row = ints[4] * 32 + iota((32, 128), 0)
    col = iota((1, 1024), 1)
    rd = [fnum((row >> (8 - 2 * k)) & 3) for k in range(TRANSMONS)]
    cd = [fnum((col >> (8 - 2 * k)) & 3) for k in range(TRANSMONS)]
    return rd, cd


def start_of(ints, gathered):
    rows = iota((8, 2), 0)
    kept = jnp.where(rows < ints[5], gathered[...], 0).astype(F32)
    return jnp.sum(jnp.sum(kept, axis=1, keepdims=True), axis=0, keepdims=True)


def drive_phase(fl, k, time):
    phi = time * fl[14 + k]
    turns = jnp.floor(phi * F32(0.5 / math.pi) + F32(0.5))
    return phi - turns * F32(6.28125) - turns * F32(2 * math.pi - 6.28125)


def energy_of(fl, digits):
    total = node_energy(fl, 0, digits[0])
    for k in range(1, TRANSMONS):
        total = total + node_energy(fl, k, digits[k])
    for k in range(TRANSMONS - 1):
        total = total + fl[5 + k] * (digits[k] * digits[k + 1])
    return total


def factor_parts(fl, span, sign, time, row_digits, col_digits):
    phis = [drive_phase(fl, k, time) for k in range(TRANSMONS)]

    def angle(digits):
        total = (F32(0.5) * span) * energy_of(fl, digits)
        drive = phis[0] * drive_weight(digits[0])
        for k in range(1, TRANSMONS):
            drive = drive + phis[k] * drive_weight(digits[k])
        return total + drive if sign > 0 else total - drive

    return sincos(angle(row_digits)), sincos(angle(col_digits))


def decay_of(fl, row_digits, col_digits):
    total = None
    for k in range(TRANSMONS):
        gap = row_digits[k] - col_digits[k]
        part = fl[9 + k] * (gap * gap)
        total = part if total is None else total + part
    return total


def start_factor(ints, fl, gathered):
    time = start_of(ints, gathered)
    rd, cd = digits_a(ints)
    phis = [drive_phase(fl, k, time) for k in range(TRANSMONS)]

    def angle(digits):
        total = phis[0] * drive_weight(digits[0])
        for k in range(1, TRANSMONS):
            total = total + phis[k] * drive_weight(digits[k])
        return total

    si, ci = sincos(angle(rd))
    sj, cj = sincos(angle(cd))
    si, ci = jnp.concatenate([si] * 8, axis=1), jnp.concatenate([ci] * 8, axis=1)
    return ci * cj + si * sj, ci * sj - si * cj


def to_rows(blocks):
    return jnp.concatenate(
        [
            blocks[:, c * 1024 + a * 256 : c * 1024 + a * 256 + 256]
            for a in range(4)
            for c in range(2)
        ],
        axis=0,
    )


def to_lanes(rows):
    return jnp.concatenate(
        [rows[(2 * a + c) * 32 : (2 * a + c) * 32 + 32, :] for c in range(2) for a in range(4)],
        axis=1,
    )


def mix_i4(o4, rows, transposed):
    parts = [
        jnp.concatenate([rows[32 * n + 8 * b : 32 * n + 8 * b + 8, :] for n in range(8)], axis=0)
        for b in range(4)
    ]
    out = []
    for a in range(4):
        total = None
        for b in range(4):
            n = 4 * b + a if transposed else 4 * a + b
            part = parts[b] * o4[n : n + 1, :]
            total = part if total is None else total + part
        out.append(total)
    return jnp.concatenate(
        [out[a][8 * n : 8 * n + 8, :] for n in range(8) for a in range(4)], axis=0
    )


def chunk_of_lane(shape):
    return (iota(shape, 1) >> 5) & 3


def send(out, offset, x):
    for c in range(2):
        for half in range(2):
            tiles = [
                x[:, c * 1024 + a * 256 + half * 128 : c * 1024 + a * 256 + half * 128 + 128]
                for a in range(4)
            ]
            chunk = chunk_of_lane((32, 128))
            for q in range(4):
                moved = [
                    tiles[a] if a == q else pltpu.roll(tiles[a], ((a - q) * 32) % 128, 1)
                    for a in range(4)
                ]
                merged = pick(chunk, moved)
                for i4 in range(4):
                    out[i4 * 8 + half * 4 + q, :, offset + c * 128 : offset + c * 128 + 128] = (
                        merged[i4 * 8 : i4 * 8 + 8, :]
                    )


def receive(ref, offset):
    chunk = chunk_of_lane((32, 128))
    pieces = {}
    for c in range(2):
        for half in range(2):
            merged = [
                jnp.concatenate(
                    [
                        ref[i4 * 8 + half * 4 + q, :, offset + c * 128 : offset + c * 128 + 128]
                        for i4 in range(4)
                    ],
                    axis=0,
                )
                for q in range(4)
            ]
            for a in range(4):
                moved = [
                    merged[q] if a == q else pltpu.roll(merged[q], ((q - a) * 32) % 128, 1)
                    for q in range(4)
                ]
                pieces[c, a, half] = pick(chunk, moved)
    return jnp.concatenate(
        [pieces[c, a, half] for c in range(2) for a in range(4) for half in range(2)], axis=1
    )


def apply_pointwise_a(rows, far, fai, conj):
    fr = jnp.concatenate([far, far], axis=1)
    fi = jnp.concatenate([fai, fai], axis=1)
    if conj:
        fi = -fi
    out = []
    for a in range(4):
        re, im = rows[64 * a : 64 * a + 32, :], rows[64 * a + 32 : 64 * a + 64, :]
        out += [re * fr - im * fi, re * fi + im * fr]
    return jnp.concatenate(out, axis=0)


def raw_kernel(x, out):
    rows = to_rows(jnp.concatenate([x[0], x[1]], axis=1))
    send(out, 0, to_lanes(pmm(pleft(row_moves(False), rows), lane_moves())))


def forward_a_kernel(
    ints, fl, gathered, gx, other, w1h, w1l, w2h, w2l, k1h, k1l, far, fai, o4, out
):
    out[:, :, 256:] = other[...]
    fr, fi = start_factor(ints, fl, gathered)
    re, im = gx[0], gx[1]
    rows = to_rows(jnp.concatenate([re * fr - im * fi, re * fi + im * fr], axis=1))
    rows = mm(left(k1h[...], k1l[...], rows), w1h[...], w1l[...])
    rows = apply_pointwise_a(rows, far[...], fai[...], False)
    send(out, 0, to_lanes(mm(mix_i4(o4, rows, False), w2h[...], w2l[...])))


def adjoint_a_kernel(
    ints, fl, pulse, gathered, y, w1h, w1l, w2h, w2l, far, fai, o4, out, t1h, t1l
):
    rows = mm(to_rows(receive(y, 0)), w2h[...], w2l[...], True)
    rows = apply_pointwise_a(mix_i4(o4, rows, True), far[...], fai[...], True)
    rows = mm(rows, w1h[...], w1l[...], True)
    lane = iota((1, 256), 1)
    sent = [
        (lane >> 6) & 3,
        ((lane >> 5) & 1) * 2 + ((lane >> 2) & 1),
        lane & 3,
        (lane >> 3) & 3,
    ]
    first = [flip(o) for o in rotations(ints, pulse, [(0, k) for k in (0, 3, 4)], 256)]
    store_kron(t1h, t1l, [first[0], identity(256), first[1], first[2]], sent)
    both = to_lanes(left(t1h[...], t1l[...], rows))
    fr, fi = first_factor(ints, fl, start_of(ints, gathered) + F32(0.5) * fnum(ints[2]))
    re, im = both[:, :1024], both[:, 1024:]
    out[0] = re * fr + im * fi
    out[1] = im * fr - re * fi


def finish_kernel(x, m, out):
    rows = pmm(to_rows(receive(m, 0)), lane_moves(), True)
    other = to_lanes(pleft(row_moves(True), rows))
    out[0] = x[0] - other[:, :1024]
    out[1] = x[1] - other[:, 1024:]


def table_b_kernel(
    ints, fl, pulse, gathered, a1h, a1l, b1h, b1l, a2h, a2l, b2h, b2l, vh, vl, fmr, fmi, ffr, ffi
):
    w = 256
    lane = iota((1, w), 1)
    natural = [(lane >> 6) & 3, (lane >> 4) & 3, (lane >> 2) & 3, lane & 3]
    eye = identity(w)
    which = [(0, k) for k in range(3)] + [(1, k) for k in range(4)]
    both = rotations(ints, pulse, which, w)
    first, second = both[:3], both[3:]
    store_kron(a1h, a1l, [*first, eye], natural)
    store_kron(b1h, b1l, [*(flip(o) for o in first), eye], natural)
    store_kron(a2h, a2l, second, natural)
    store_kron(b2h, b2l, [flip(o) for o in second], natural)
    row = iota((16, w), 0)
    cl, l0, l1, l2, ll = (lane >> 7), (lane >> 5) & 3, (lane >> 3) & 3, (lane >> 1) & 3, lane & 1
    t0 = lane_rows(flip(second[0]), l0)
    t1 = lane_rows(flip(second[1]), l1)
    t2 = lane_rows(flip(second[2]), l2)
    low = pick((row >> 1) & 3, t2) * jnp.where((row & 1) == ll, F32(1.0), F32(0.0))
    high_bit = row >> 3
    for n in range(16):
        c, d0, top = n >> 3, (n >> 1) & 3, n & 1
        mid = jnp.where(high_bit == 0, t1[2 * top], t1[2 * top + 1])
        block = low * mid * (t0[d0] * jnp.where(cl == c, F32(1.0), F32(0.0)))
        hi, lo = split(block)
        vh[16 * n : 16 * n + 16, :] = hi
        vl[16 * n : 16 * n + 16, :] = lo
    row = iota((256, 128), 0)
    col = iota((1, 128), 1)
    rd = [fnum((row >> (6 - 2 * k)) & 3) for k in range(4)]
    cd = [fnum((col >> 5) & 3), fnum((col >> 3) & 3), fnum((col >> 1) & 3)]
    t12 = F32(0.5) * (fnum(ints[2]) + fnum(ints[3]))

    def node(k, n):
        return node_energy(fl, k, n) + fl[14 + k] * drive_weight(n)

    ai = fl[5] * (rd[0] * rd[1]) + fl[6] * (rd[1] * rd[2]) + fl[7] * (rd[2] * rd[3])
    for k in range(4):
        ai = ai + node(k, rd[k])
    aj = fl[5] * (cd[0] * cd[1]) + fl[6] * (cd[1] * cd[2])
    for k in range(3):
        aj = aj + node(k, cd[k])
    gap = None
    for k in range(3):
        part = fl[9 + k] * ((rd[k] - cd[k]) * (rd[k] - cd[k]))
        gap = part if gap is None else gap + part
    mag = jnp.exp(-t12 * gap)
    si, ci = sincos(t12 * ai)
    sj, cj = sincos(t12 * aj)
    fmr[...] = mag * (ci * cj + si * sj)
    fmi[...] = mag * (ci * sj - si * cj)
    rank = ints[4]
    i4 = fnum(jnp.full((256, 128), rank >> 3, jnp.int32))
    j3 = fnum(jnp.full((1, 128), (rank >> 1) & 3, jnp.int32))
    j4 = fnum((rank & 1) * 2 + (col & 1))
    rows = [*rd, i4]
    cols = [*cd, j3, j4]
    span = fnum(ints[3])
    time = start_of(ints, gathered) + (fnum(ints[2]) + F32(0.5) * span)
    (si, ci), (sj, cj) = factor_parts(fl, span, -1, time, rows, cols)
    mag = jnp.exp(F32(-0.5) * span * decay_of(fl, rows, cols))
    ffr[...] = mag * (ci * cj + si * sj)
    ffi[...] = mag * (ci * sj - si * cj)


def cmul(x, fr, fi, conj=False):
    re, im = x[:, :128], x[:, 128:]
    if conj:
        return jnp.concatenate([re * fr + im * fi, im * fr - re * fi], axis=1)
    return jnp.concatenate([re * fr - im * fi, re * fi + im * fr], axis=1)


def both_b_kernel(x, a1h, a1l, b1h, b1l, a2h, a2l, b2h, b2l, vh, vl, fmr, fmi, ffr, ffi, out):
    z = left(a1h[...], a1l[...], x[:, :256])
    z = cmul(z, fmr[...], fmi[...])
    z = left(a2h[...], a2l[...], z)
    z = mm(z, vh[...], vl[...])
    z = cmul(z, ffr[...], ffi[...]) - x[:, 256:]
    out[:, 256:] = z
    z = cmul(z, ffr[...], ffi[...], True)
    z = left(b2h[...], b2l[...], z)
    z = mm(z, vh[...], vl[...], True)
    z = cmul(z, fmr[...], fmi[...], True)
    out[:, :256] = left(b1h[...], b1l[...], z)


SMEM = pl.BlockSpec(memory_space=pltpu.SMEM)
VMEM = pl.BlockSpec(memory_space=pltpu.VMEM)
HBM = pl.BlockSpec(memory_space=pltpu.MemorySpace.HBM)


def with_params(kernel):
    def run(segment, tick, rank, shift, coupling, dephase, detuning, *refs):
        ints = [segment[0, 0], segment[0, 1], tick[0, 0], tick[0, 1], rank[0], rank[1]]
        sources = ((shift, 5), (coupling, 4), (dephase, 5), (detuning, 5))
        kernel(ints, [ref[n] for ref, count in sources for n in range(count)], *refs)

    return run


def call(kernel, args, scalars, outs, flops, name, far=(), scratch=()):
    specs = [SMEM if n < scalars else HBM if n in far else VMEM for n in range(len(args))]
    return pl.pallas_call(
        with_params(kernel) if scalars else kernel,
        in_specs=specs,
        out_specs=jax.tree.map(lambda _: VMEM, outs),
        out_shape=outs,
        scratch_shapes=scratch,
        name=name,
        compiler_params=pltpu.CompilerParams(vmem_limit_bytes=16 << 20),
        cost_estimate=pl.CostEstimate(flops=flops, transcendentals=0, bytes_accessed=1 << 20),
    )(*args)


def sds(*shape, dtype=F32):
    return jax.ShapeDtypeStruct(shape, dtype)


def local(linkage, pulse, segments, ticks, detuning, level_shift, coupling, dephase):
    current = linkage[:, 0]
    phases = lax.axis_size("phase")
    rank = jnp.stack([lax.axis_index("row"), lax.axis_index("phase")]).astype(jnp.int32)
    params = (segments, ticks, rank, level_shift, coupling, dephase, detuning)
    angles = jnp.transpose(pulse, (1, 2, 0))
    gathered = lax.all_to_all(
        jnp.broadcast_to(ticks, (phases, STEPS)), "phase", split_axis=0, concat_axis=0, tiled=True
    )
    def turn(x):
        return lax.all_to_all(
            x.reshape(32, 8, 512), "row", split_axis=0, concat_axis=0, tiled=True
        )

    following = lax.ppermute(current, "phase", [((i + 1) % phases, i) for i in range(phases)])
    following = call(raw_kernel, (following,), 0, sds(32, 8, 256), 1 << 26, "raw")
    square = sds(256, 256, dtype=BF16)
    *tables_a, weighed = call(
        table_a_kernel,
        (
            *params,
            angles,
            pltpu.with_memory_space_constraint(current, pltpu.MemorySpace.HBM),
        ),
        8,
        (
            *([square] * 6),
            sds(32, 128),
            sds(32, 128),
            sds(16, 256),
            sds(2, 32, 1024),
        ),
        1 << 28,
        "table_a",
        far=(8,),
        scratch=(pltpu.VMEM((2, 32, 1024), F32), pltpu.SemaphoreType.DMA),
    )
    sent = call(
        forward_a_kernel,
        (*params, gathered, weighed, following, *tables_a),
        7,
        sds(32, 8, 512),
        1 << 28,
        "forward_a",
    )
    turned = turn(sent)
    tables_b = call(
        table_b_kernel,
        (*params, angles, gathered),
        8,
        (*([square] * 10), *([sds(256, 128)] * 4)),
        1 << 28,
        "table_b",
    )
    back = call(
        both_b_kernel,
        (turned.reshape(256, 512), *tables_b),
        0,
        sds(256, 512),
        1 << 28,
        "both_b",
    )
    returned = turn(back)
    earlier = lax.ppermute(
        returned[:, :, 256:], "phase", [(i, (i + 1) % phases) for i in range(phases)]
    )
    costate = call(
        adjoint_a_kernel,
        (*params, angles, gathered, returned, *tables_a[:4], *tables_a[6:]),
        8,
        sds(2, 32, 1024),
        1 << 28,
        "adjoint_a",
        scratch=(pltpu.VMEM((256, 256), BF16), pltpu.VMEM((256, 256), BF16)),
    )
    result = call(finish_kernel, (costate, earlier), 0, sds(2, 32, 1024), 1 << 26, "finish")
    return result[:, None]


def solution(mesh):
    return jax.shard_map(
        local,
        mesh=mesh,
        in_specs=(
            P(None, "phase", "row", None),
            P(),
            P("phase", None),
            P("phase", None),
            P(),
            P(),
            P(),
            P(),
        ),
        out_specs=P(None, "phase", "row", None),
        check_vma=False,
    )
```
